256 devices in a mesh: seq: 32 (over x, z_hi, y), tp: 8 (over z_lo, core).
Axes of the slice: x: 4, y: 4, z: 8 (z_hi: 2, z_lo: 4; z = z_hi * 4 + z_lo), core: 2. Of those that a mesh axis runs over, the one named last changes fastest.
Arguments:
- latent: bfloat16 [2, 32, 1024, 1152], P(None, 'seq', 'tp'), may hold values from -6 to 6
- modulation: float32 [2, 9, 1152], replicated, may hold values from -4 to 4
- qkv_spatial: bfloat16 [3, 1152, 1152], P(None, None, 'tp'), may hold values from -0.1875 to 0.1875
- gain_spatial: float32 [2, 72], replicated, may hold values from 0.5 to 1.7
- out_spatial: bfloat16 [1152, 1152], P('tp'), may hold values from -0.1875 to 0.1875
- qkv_temporal: bfloat16 [3, 1152, 1152], P(None, None, 'tp'), may hold values from -0.1875 to 0.1875
- gain_temporal: float32 [2, 72], replicated, may hold values from 0.5 to 1.7
- out_temporal: bfloat16 [1152, 1152], P('tp'), may hold values from -0.1875 to 0.1875
- fc_in: bfloat16 [1152, 4608], P(None, 'tp'), may hold values from -0.1875 to 0.1875
- fc_out: bfloat16 [4608, 1152], P('tp'), may hold values from -0.09375 to 0.09375
Outputs:
- result: bfloat16 [2, 32, 1024, 1152], P(None, 'seq', 'tp')
The draws below stay inside these ranges and needn't reach their ends.
All inputs are finite; a program needn't handle non-finite values.
Results may differ from the reference program's by a relative error of at most 0.017.
Values may be sent and summed in bfloat16 or wider, within the bound.
A program may use at most 64 MiB of HBM per device.

```python
import math
import jax
import jax.numpy as jnp
from jax import lax

D = 1152
H = 16
FF = 4608
HD = 72
B = 2
P_SIZE = 1024
F = 32
N_TP = 8


def steps_of(rng, extent, split, low, top_value):
    def one(dim, shards_of):
        draws = jax.random.uniform(jax.random.fold_in(jax.random.fold_in(rng, 6), dim), (shards_of,), jnp.float32, low / len(split), top_value / len(split))
        return jnp.repeat(jnp.exp(draws), extent[dim] // shards_of).reshape((-1,) + (1,) * (len(extent) - dim - 1))

    loudness = one(*split[0])
    for cut in split[1:]:
        loudness = loudness * one(*cut)
    return loudness


def bell_draw(key, shape, width, reach, cuts=(), held_as=jnp.bfloat16):
    result = width * jax.random.normal(key, shape, jnp.float32)
    if cuts:
        result = result * steps_of(key, shape, cuts, -0.22, 0.18)
    return jnp.clip(result, -reach, reach).astype(held_as)


def setup_inputs(seed: int = 0) -> dict:
    seeds = jax.random.split(jax.random.key(seed), 11)
    return {
        "latent": bell_draw(seeds[0], (B, F, P_SIZE, D), 1.0, 6.0, ((1, 32), (2, 8))),
        "modulation": bell_draw(seeds[1], (B, 9, D), 0.7, 4.0, (), jnp.float32),
        "qkv_spatial": bell_draw(seeds[2], (3, D, D), D ** -0.5, 0.1875, ((2, 8),)),
        "gain_spatial": jnp.clip(jax.random.uniform(seeds[3], (2, HD), jnp.float32, 0.5, 1.7), 0.5, 1.7),
        "out_spatial": bell_draw(seeds[4], (D, D), D ** -0.5, 0.1875, ((0, 8),)),
        "qkv_temporal": bell_draw(seeds[5], (3, D, D), D ** -0.5, 0.1875, ((2, 8),)),
        "gain_temporal": jnp.clip(jax.random.uniform(seeds[6], (2, HD), jnp.float32, 0.5, 1.7), 0.5, 1.7),
        "out_temporal": bell_draw(seeds[7], (D, D), D ** -0.5, 0.1875, ((0, 8),)),
        "fc_in": bell_draw(seeds[8], (D, FF), D ** -0.5, 0.1875, ((1, 8),)),
        "fc_out": bell_draw(seeds[9], (FF, D), FF ** -0.5, 0.09375, ((0, 8),)),
    }


epsilon = 1e-06

def layer_norm(values):
    average = lax.optimization_barrier(jnp.mean(values, axis=-1, keepdims=True))
    centred = values - average
    variance = lax.optimization_barrier(jnp.mean(centred * centred, axis=-1, keepdims=True))
    return centred * lax.rsqrt(variance + epsilon)

def modulated(field, modulation, offset):
    shift_row = modulation[:, offset][:, None, None, :]
    scale_row = modulation[:, offset + 1][:, None, None, :]
    return (layer_norm(field) * (1.0 + scale_row) + shift_row).astype(jnp.bfloat16)

def project_rows(normed, table, gains, head_dim):
    flat = normed.reshape(-1, normed.shape[-1])
    results = []
    for which_part in range(3):
        projected = jnp.dot(flat, table[which_part], preferred_element_type=jnp.float32)
        if which_part < 2:
            shaped = projected.reshape(projected.shape[0], -1, head_dim)
            shaped = shaped * lax.rsqrt(lax.optimization_barrier(jnp.mean(shaped * shaped, axis=-1, keepdims=True)) + epsilon) * gains[which_part]
            projected = shaped.reshape(projected.shape)
        results.append(projected.astype(jnp.bfloat16).reshape(normed.shape[:-1] + (table.shape[-1],)))
    return results

def attend_one(members, head_dim):
    query_rows, key_rows, value_rows = members
    length, feature_width = query_rows.shape
    head_count = feature_width // head_dim
    query_heads = query_rows.astype(jnp.float32).reshape(length, head_count, head_dim)
    key_heads = key_rows.astype(jnp.float32).reshape(length, head_count, head_dim)
    value_heads = value_rows.astype(jnp.float32).reshape(length, head_count, head_dim)
    scores = jnp.einsum('qhe,khe->hqk', query_heads, key_heads) / math.sqrt(head_dim)
    weights = jnp.exp(scores)
    probabilities = (weights / lax.optimization_barrier(jnp.sum(weights, axis=-1, keepdims=True))).astype(jnp.bfloat16)
    probabilities = lax.optimization_barrier(probabilities).astype(jnp.float32)
    mixed_heads = jnp.einsum('hqk,khe->qhe', probabilities, value_heads)
    return mixed_heads.reshape(length, feature_width).astype(jnp.bfloat16)

def grouped_product(left, right):
    flat = left.reshape(-1, left.shape[-1])
    group_width = flat.shape[1] // N_TP
    total = jnp.zeros((flat.shape[0], right.shape[1]), jnp.float32)
    for group_index in range(N_TP):
        lower = group_index * group_width
        piece_sum = jnp.dot(flat[:, lower:lower + group_width], right[lower:lower + group_width], preferred_element_type=jnp.float32)
        rounded = lax.optimization_barrier(piece_sum.astype(jnp.bfloat16))
        total = total + rounded.astype(jnp.float32)
    return total.astype(jnp.bfloat16).reshape(left.shape[:-1] + (right.shape[1],))

def reference(latent, modulation, qkv_spatial, gain_spatial, out_spatial, qkv_temporal, gain_temporal, out_temporal, fc_in, fc_out):
    head_dim = D // H
    batches, frames, patches, feature_width = latent.shape
    running = latent.astype(jnp.float32)
    normed = modulated(running, modulation, 0)
    query_rows, key_rows, value_rows = project_rows(normed, qkv_spatial, gain_spatial, head_dim)
    grouped = tuple((item.reshape(batches * frames, patches, feature_width) for item in (query_rows, key_rows, value_rows)))
    mixed_heads = lax.map(lambda members: attend_one(members, head_dim), grouped).reshape(batches, frames, patches, feature_width)
    spatial_out = grouped_product(mixed_heads, out_spatial)
    running = running + modulation[:, 2][:, None, None, :] * spatial_out.astype(jnp.float32)
    normed = modulated(running, modulation, 3)
    query_rows, key_rows, value_rows = project_rows(normed, qkv_temporal, gain_temporal, head_dim)
    grouped = tuple((item.transpose(0, 2, 1, 3).reshape(batches * patches, frames, feature_width) for item in (query_rows, key_rows, value_rows)))
    mixed_heads = lax.map(lambda members: attend_one(members, head_dim), grouped)
    mixed_heads = mixed_heads.reshape(batches, patches, frames, feature_width).transpose(0, 2, 1, 3)
    temporal_out = grouped_product(mixed_heads, out_temporal)
    running = running + modulation[:, 5][:, None, None, :] * temporal_out.astype(jnp.float32)
    normed = modulated(running, modulation, 6)
    flat = normed.reshape(-1, feature_width)
    hidden = jax.nn.gelu(jnp.dot(flat, fc_in, preferred_element_type=jnp.float32), approximate=True).astype(jnp.bfloat16)
    mlp_out = grouped_product(hidden, fc_out).reshape(batches, frames, patches, feature_width)
    return (running + modulation[:, 8][:, None, None, :] * mlp_out.astype(jnp.float32)).astype(jnp.bfloat16)
```

```python
import math

import jax
import jax.numpy as jnp
from jax import lax
from jax.experimental import pallas as pl
from jax.experimental.pallas import tpu as pltpu
from jax.sharding import PartitionSpec as P

D = 1152
H = 16
HD = 72
HW = 144
N_TP = 8
N_SEQ = 32
ROUNDS = 4
MESH = pl.DeviceIdType.MESH
EPS = 1e-06
SCALE = 1.0 / math.sqrt(HD)
F32 = jnp.float32
BF16 = jnp.bfloat16

O_S, QKV_T, O_T, FC1, FC2, END = 0, 9, 36, 45, 81, 117


def layer_norm(values):
    average = jnp.mean(values, axis=-1, keepdims=True)
    centred = values - average
    variance = jnp.mean(centred * centred, axis=-1, keepdims=True)
    return centred * lax.rsqrt(variance + EPS)


def dot(left, right, left_dim=1, right_dim=0):
    return lax.dot_general(
        left, right, (((left_dim,), (right_dim,)), ((), ())), preferred_element_type=F32
    )


def head_norm_rows(values, gain):
    halves = []
    for head in range(2):
        part = values[head * HD : (head + 1) * HD]
        halves.append(part * lax.rsqrt(jnp.mean(part * part, axis=0, keepdims=True) + EPS))
    return jnp.concatenate(halves, axis=0) * gain


def head_norm_lanes(values, gain):
    first = lax.broadcasted_iota(jnp.int32, values.shape, 1) < HD
    square = values * values
    low = jnp.sum(jnp.where(first, square, 0.0), axis=-1, keepdims=True)
    high = jnp.sum(jnp.where(first, 0.0, square), axis=-1, keepdims=True)
    factor = jnp.where(
        first, lax.rsqrt(low * (1.0 / HD) + EPS), lax.rsqrt(high * (1.0 / HD) + EPS)
    )
    return values * factor * gain


def remote(src, dst, send_sem, recv_sem, seq, tp):
    return pltpu.make_async_remote_copy(
        src_ref=src,
        dst_ref=dst,
        send_sem=send_sem,
        recv_sem=recv_sem,
        device_id={"seq": seq, "tp": tp},
        device_id_type=MESH,
    )


def greet(peers):
    barrier = pltpu.get_barrier_semaphore()
    for seq, tp in peers:
        pl.semaphore_signal(
            barrier, inc=1, device_id={"seq": seq, "tp": tp}, device_id_type=MESH
        )
    pl.semaphore_wait(barrier, len(peers))


def spatial_kernel(
    lat,
    mod,
    wqkv,
    gcol,
    grow,
    wsh,
    mid,
    nrm,
    g,
    xs,
    ks,
    qs,
    vs,
    ot,
    heads,
    wos,
    ag_send,
    ag_recv,
    s1_send,
    s1_recv,
    own_sem,
    w_send,
    w_recv,
    d_send,
    d_recv,
    h_send,
    h_recv,
    os_sem,
):
    seq, me = lax.axis_index("seq"), lax.axis_index("tp")
    x, zh, y = seq // 8, lax.rem(seq // 4, 2), lax.rem(seq, 4)
    zl, c = me // 2, lax.rem(me, 2)
    sib = zl * 2 + (1 - c)

    def xy(dx, dy):
        return (lax.rem(x + dx + 4, 4) * 2 + zh) * 4 + lax.rem(y + dy + 4, 4)

    def zdev(dz, core):
        z = lax.rem(zh * 4 + zl + dz + 8, 8)
        return (x * 2 + z // 4) * 4 + y, lax.rem(z, 4) * 2 + core

    ring = (xy(1, 0), xy(-1, 0), xy(0, 1), xy(0, -1))
    z_targets = [zdev(dz, core) for dz in (1, -1, 2) for core in range(2)]
    peers = [(seq, lax.rem(me + i, N_TP)) for i in range(1, N_TP)]
    peers += [(to, me) for to in ring]
    peers += [zdev(dz, core) for dz in (1, -1, 2, -2) for core in range(2)]
    greet(peers)

    def s1_copies(k):
        copies = []
        for i, (to_seq, to_tp) in enumerate(z_targets):
            unit = (x * 4 + y) * 2 + i % 2
            copies.append(
                remote(
                    wsh.at[k, unit],
                    g.at[me, k, x, y, i % 2],
                    s1_send.at[k, i],
                    s1_recv.at[k, me],
                    to_seq,
                    to_tp,
                )
            )
        copies.append(
            remote(
                wsh.at[k, (x * 4 + y) * 2 + (1 - c)],
                g.at[me, k, x, y, 1 - c],
                s1_send.at[k, 6],
                s1_recv.at[k, me],
                seq,
                sib,
            )
        )
        return copies

    def own_copy(k):
        return pltpu.make_async_copy(
            wsh.at[k, (x * 4 + y) * 2 + c], g.at[me, k, x, y, c], own_sem.at[k]
        )

    def s1_start(k):
        own_copy(k).start()
        for copy in s1_copies(k):
            copy.start()

    def s1_wait(k):
        own_copy(k).wait()
        for i in range(1, N_TP):
            source = lax.rem(me + i, N_TP)
            spot = g.at[source, k, x, y, c]
            remote(spot, spot, s1_send.at[k, 0], s1_recv.at[k, source], seq, sib).wait_recv()

    left, right = pl.ds(0, 4), pl.ds(4, 4)
    x_back, x_next = lax.rem(x + 3, 4), lax.rem(x + 1, 4)
    y_back, y_next = lax.rem(y + 3, 4), lax.rem(y + 1, 4)

    def ring_copies(stage, k):
        if stage == 0:
            spots = [g.at[left, k, x, y, c]] * 2 + [g.at[right, k, x, y, c]] * 2
        elif stage == 1:
            spots = [
                g.at[pl.ds(0, 2), k, x_back, y, c],
                g.at[pl.ds(2, 2), k, x_next, y, c],
                g.at[pl.ds(4, 2), k, x, y_back, c],
                g.at[pl.ds(6, 2), k, x, y_next, c],
            ]
        elif stage == 2:
            spots = [g.at[right, k, x, :, c]] * 2 + [g.at[left, k, :, y, c]] * 2
        else:
            spots = [
                g.at[pl.ds(4, 2), k, x_back, :, c],
                g.at[pl.ds(6, 2), k, x_next, :, c],
                g.at[pl.ds(0, 2), k, :, y_back, c],
                g.at[pl.ds(2, 2), k, :, y_next, c],
            ]
        return [
            remote(spot, spot, w_send.at[stage, k, i], w_recv.at[stage, k, i], ring[i], me)
            for i, spot in enumerate(spots)
        ]

    def ring_start(stage, k):
        for copy in ring_copies(stage, k):
            copy.start()

    def ring_wait(stage, k):
        for copy in ring_copies(stage, k):
            copy.wait_recv()

    def core_copy(k):
        spot = g.at[:, k, :, :, c]
        return remote(spot, spot, d_send.at[k], d_recv.at[k], seq, sib)

    def pump(step, k):
        if step == 0:
            s1_start(k)
        elif step == 1:
            s1_wait(k)
            ring_start(0, k)
        elif step <= 4:
            ring_wait(step - 2, k)
            ring_start(step - 1, k)
        elif step == 5:
            ring_wait(3, k)
            core_copy(k).start()
        else:
            core_copy(k).wait_recv()

    def ag_copy(slot, b, way):
        to = (jnp.minimum(zl + 1, 3) * 2 + c, jnp.maximum(zl - 1, 0) * 2 + c, sib)[way]
        spot = xs.at[slot, b]
        return remote(spot, spot, ag_send.at[slot, b, way], ag_recv.at[slot, b], seq, to)

    def ag_step(distance, b, what):
        for way in range(2):
            origin = zl - distance if way == 0 else zl + distance
            there = (zl >= distance) if way == 0 else (zl + distance <= 3)
            more = (zl < 3) if way == 0 else (zl > 0)
            if distance == 0:
                there = more
            slot = origin * 2 + c

            @pl.when(there)
            def _():
                if what == 0 and distance > 0:
                    ag_copy(slot, b, 2).wait_recv()
                if distance == 0:
                    copy = ag_copy(slot, b, way)
                    copy.start() if what == 0 else copy.wait_send()
                else:

                    @pl.when(more)
                    def _():
                        copy = ag_copy(slot, b, way)
                        copy.start() if what == 0 else copy.wait_send()

                    copy = ag_copy(slot, b, 2)
                    copy.start() if what == 0 else copy.wait_send()

        if distance == 0:
            copy = ag_copy(me, b, 2)
            copy.start() if what == 0 else copy.wait_send()

    def project(z):
        rows = xs[pl.ds(z * 2, 2)].reshape(512, D)
        queries = head_norm_rows(dot(wqkv[0], rows, 1, 1), gcol[...]).astype(BF16)
        values = dot(wqkv[2], rows, 1, 1).astype(BF16)
        keys = head_norm_lanes(dot(rows, wqkv[1], 1, 1), grow[...]).astype(BF16)
        for core in range(2):
            for b in range(2):
                at = (core * 2 + b) * 128
                qs[b, z * 2 + core] = queries[:, at : at + 128]
                spot = pl.ds(pl.multiple_of((z * 2 + core) * 128, 128), 128)
                vs[b, :, spot] = values[:, at : at + 128]
                ks[b, z * 2 + core] = keys[at : at + 128]

    def head_copy(b, to):
        return remote(
            ot.at[b, to], heads.at[b, me], h_send.at[b, to], h_recv.at[b, me], seq, to
        )

    def attend(b):
        keys = ks[b].reshape(N_TP * 128, HW)
        values = vs[b]

        def block(i, _):
            to = lax.rem(me + 1 + i, N_TP)
            query = qs[b, to]
            zero = jnp.zeros((HD, 128), BF16)
            pair = jnp.concatenate(
                [
                    jnp.concatenate([query[:HD].astype(F32), zero.astype(F32)], axis=0),
                    jnp.concatenate([zero.astype(F32), query[HD:].astype(F32)], axis=0),
                ],
                axis=1,
            ).astype(BF16)
            weights = jnp.exp(dot(keys, pair) * SCALE)
            total = jnp.sum(weights, axis=0, keepdims=True)
            mixed = dot(values, weights.astype(BF16)) / total
            result = jnp.concatenate([mixed[:HD, :128], mixed[HD:, 128:]], axis=0).astype(BF16)

            @pl.when(to != me)
            def _():
                ot[b, to] = result
                head_copy(b, to).start()

            @pl.when(to == me)
            def _():
                heads[b, me] = result

            return 0

        lax.fori_loop(0, N_TP, block, 0)

    def finish(b):
        for i in range(1, N_TP):
            source = lax.rem(me + i, N_TP)
            spot = heads.at[b, source]
            remote(spot, spot, h_send.at[b, source], h_recv.at[b, source], seq, source).wait_recv()
        mixed = heads[b].reshape(D, 128).T
        out = dot(mixed, wos[...].reshape(D, D)).astype(BF16).astype(F32)
        rows = pl.ds(b * 128, 128)
        late = lat[rows].astype(F32) + mod[b, 2:3] * out
        mid[rows] = late
        normed = layer_norm(late) * (1.0 + mod[b, 4:5]) + mod[b, 3:4]
        nrm[pl.ds(b * 16, 16)] = normed.reshape(16, 8, D).astype(BF16)

    pump(0, 0)
    for b in range(2):
        rows = lat[pl.ds(b * 128, 128)].astype(F32)
        xs[me, b] = (layer_norm(rows) * (1.0 + mod[b, 1:2]) + mod[b, 0:1]).astype(BF16)
        ag_step(0, b, 0)
    pump(0, 1)
    for b in range(2):
        ag_copy(sib, b, 2).wait_recv()
    project(zl)
    pump(1, 0)
    ag_step(1, 0, 0)
    pump(2, 0)
    ag_step(1, 1, 0)
    pump(0, 2)
    pump(1, 1)
    pump(3, 0)
    ag_step(2, 0, 0)
    pump(0, 3)
    pump(2, 1)
    ag_step(2, 1, 0)
    pump(3, 1)
    pump(1, 2)
    pump(4, 0)
    ag_step(3, 0, 0)
    pump(2, 2)
    ag_step(3, 1, 0)
    for distance in range(1, 4):
        for b in range(2):
            other = lax.rem(zl + distance, 4) * 2 + (1 - c)
            ag_copy(other, b, 2).wait_recv()
    for i in range(1, 4):
        project(lax.rem(zl + i, 4))
    pump(1, 3)
    attend(0)
    pump(5, 0)
    pump(4, 1)
    pump(3, 2)
    pump(2, 3)
    attend(1)
    pump(6, 0)
    os_copies = [
        pltpu.make_async_copy(g.at[:, 0, 0, i], wos.at[:, pl.ds(2 * i, 2)], os_sem.at[i])
        for i in range(4)
    ] + [pltpu.make_async_copy(g.at[:, 0, 1, 0, 0], wos.at[:, 8], os_sem.at[4])]
    for copy in os_copies:
        copy.start()
    for copy in os_copies:
        copy.wait()
    finish(0)
    finish(1)
    pump(5, 1)
    pump(4, 2)
    pump(3, 3)
    pump(6, 1)
    pump(5, 2)
    pump(4, 3)
    pump(6, 2)
    pump(5, 3)
    pump(6, 3)

    for b in range(2):
        for distance in range(4):
            ag_step(distance, b, 1)
        for i in range(1, N_TP):
            head_copy(b, lax.rem(me + i, N_TP)).wait_send()
    for k in range(ROUNDS):
        for copy in s1_copies(k):
            copy.wait_send()
        for stage in range(4):
            for copy in ring_copies(stage, k):
                copy.wait_send()
        core_copy(k).wait_send()


def temporal_kernel(
    nrm,
    mid,
    mod,
    gcol,
    grow,
    g,
    result,
    rows_in,
    rows_out,
    rows_back,
    ot,
    wqkv,
    wo,
    w1,
    w2,
    late,
    f_send,
    f_recv,
    b_send,
    b_recv,
    w_sem,
):
    seq, me = lax.axis_index("seq"), lax.axis_index("tp")
    loads = [
        pltpu.make_async_copy(g.at[:, pl.ds(QKV_T, 27)], wqkv, w_sem.at[0]),
        pltpu.make_async_copy(g.at[:, pl.ds(O_T, 9)], wo, w_sem.at[1]),
        pltpu.make_async_copy(g.at[:, pl.ds(FC1, 36)], w1, w_sem.at[2]),
        pltpu.make_async_copy(g.at[:, pl.ds(FC2, 36)], w2, w_sem.at[3]),
    ]
    for load in loads:
        load.start()
    greet([(lax.rem(seq + i, N_SEQ), me) for i in range(1, N_SEQ)])

    def exchange(source, target, send, recv):
        def start(i, _):
            to = lax.rem(seq + i, N_SEQ)
            remote(source.at[to], target.at[seq], send.at[to], recv.at[seq], to, me).start()
            return 0

        lax.fori_loop(1, N_SEQ, start, 0)
        target[seq] = source[seq]

        def finish(i, _):
            sender = lax.rem(seq + i, N_SEQ)
            spot = target.at[sender]
            remote(spot, spot, send.at[sender], recv.at[sender], sender, me).wait_recv()
            return 0

        lax.fori_loop(1, N_SEQ, finish, 0)

    def drain(source, send, recv):
        def finish(i, _):
            to = lax.rem(seq + i, N_SEQ)
            spot = source.at[to]
            remote(spot, spot, send.at[to], recv.at[to], to, me).wait_send()
            return 0

        lax.fori_loop(1, N_SEQ, finish, 0)

    exchange(nrm, rows_in, f_send, f_recv)
    rows = rows_in[...].astype(F32).reshape(256, D).astype(BF16)
    same = (
        lax.rem(lax.broadcasted_iota(jnp.int32, (256, 256), 0), 8)
        == lax.rem(lax.broadcasted_iota(jnp.int32, (256, 256), 1), 8)
    )
    loads[0].wait()

    def pair_of_heads(t, _):
        weights = wqkv[t].reshape(3 * HW, D)
        queries = head_norm_rows(dot(weights[:HW], rows, 1, 1), gcol[...])
        keys = head_norm_lanes(dot(rows, weights[HW : 2 * HW], 1, 1), grow[...]).astype(BF16)
        values = dot(weights[2 * HW :], rows, 1, 1).astype(BF16)
        parts = []
        zero = jnp.zeros((HD, 256), F32)
        for head in range(2):
            kept = queries[head * HD : (head + 1) * HD]
            kept = jnp.concatenate([kept, zero] if head == 0 else [zero, kept], axis=0)
            scores = dot(keys, kept.astype(BF16)) * SCALE
            probs = jnp.where(same, jnp.exp(scores), 0.0)
            total = jnp.sum(probs, axis=0, keepdims=True)
            mixed = dot(values, probs.astype(BF16)) / total
            parts.append(mixed[head * HD : (head + 1) * HD])
        ot[t] = jnp.concatenate(parts, axis=0).astype(BF16)
        return 0

    lax.fori_loop(0, N_TP, pair_of_heads, 0)
    loads[1].wait()
    mixed = ot[...].reshape(D, 256).T
    out = dot(mixed, wo[...].reshape(D, D))
    rows_out[...] = out.reshape(N_SEQ, 8, D).astype(BF16)
    exchange(rows_out, rows_back, b_send, b_recv)
    back = rows_back[...].astype(F32).reshape(256, D)
    normed = []
    for b in range(2):
        part = mid[pl.ds(b * 128, 128)] + mod[b, 5:6] * back[b * 128 : (b + 1) * 128]
        late[pl.ds(b * 128, 128)] = part
        normed.append(layer_norm(part) * (1.0 + mod[b, 7:8]) + mod[b, 6:7])
    normed = jnp.concatenate(normed, axis=0).astype(BF16)
    loads[2].wait()
    loads[3].wait()

    def hidden_chunk(t, total):
        u = dot(normed, w1[t].reshape(576, D), 1, 1)
        h = 0.5 * u * (1.0 + jnp.tanh(math.sqrt(2.0 / math.pi) * (u + 0.044715 * (u * u * u))))
        return total + dot(h.astype(BF16), w2[t].reshape(576, D))

    total = lax.fori_loop(0, N_TP, hidden_chunk, jnp.zeros((256, D), F32))
    total = total.astype(BF16).astype(F32)
    for b in range(2):
        at = pl.ds(b * 128, 128)
        result[at] = (late[at] + mod[b, 8:9] * total[b * 128 : (b + 1) * 128]).astype(BF16)
    drain(nrm, f_send, f_recv)
    drain(rows_out, b_send, b_recv)


def body(
    latent,
    modulation,
    qkv_spatial,
    gain_spatial,
    out_spatial,
    qkv_temporal,
    gain_temporal,
    out_temporal,
    fc_in,
    fc_out,
):
    def gains(table):
        column = jnp.tile(table[0], 2).reshape(HW, 1)
        row = jnp.tile(table[1], 2).reshape(1, HW)
        return column, row

    sizes = (144, 432, 144, 576, 576)
    pieces = [
        out_spatial,
        qkv_temporal.transpose(0, 2, 1).reshape(432, D),
        out_temporal,
        fc_in.T,
        fc_out,
        jnp.zeros((2048 - sum(sizes), D), BF16),
    ]
    wsh = jnp.concatenate(pieces, axis=0).reshape(ROUNDS, 32, 16, D)
    vmem = pl.BlockSpec(memory_space=pltpu.VMEM)
    hbm = pl.BlockSpec(memory_space=pl.ANY)
    dma = pltpu.SemaphoreType.DMA
    gcol, grow = gains(gain_spatial)
    mid, nrm, g = pl.pallas_call(
        spatial_kernel,
        name="spatial",
        out_shape=(
            jax.ShapeDtypeStruct((256, D), F32),
            jax.ShapeDtypeStruct((N_SEQ, 8, D), BF16),
            jax.ShapeDtypeStruct((N_TP, ROUNDS, 4, 4, 2, 16, D), BF16),
        ),
        in_specs=[vmem] * 5 + [hbm],
        out_specs=(vmem, vmem, hbm),
        scratch_shapes=[
            pltpu.VMEM((N_TP, 2, 128, D), BF16),
            pltpu.VMEM((2, N_TP, 128, HW), BF16),
            pltpu.VMEM((2, N_TP, HW, 128), BF16),
            pltpu.VMEM((2, HW, 1024), BF16),
            pltpu.VMEM((2, N_TP, HW, 128), BF16),
            pltpu.VMEM((2, N_TP, HW, 128), BF16),
            pltpu.VMEM((N_TP, 9, 16, D), BF16),
            dma((N_TP, 2, 3)),
            dma((N_TP, 2)),
            dma((ROUNDS, 7)),
            dma((ROUNDS, N_TP)),
            dma((ROUNDS,)),
            dma((4, ROUNDS, 4)),
            dma((4, ROUNDS, 4)),
            dma((ROUNDS,)),
            dma((ROUNDS,)),
            dma((2, N_TP)),
            dma((2, N_TP)),
            dma((5,)),
        ],
        compiler_params=pltpu.CompilerParams(
            collective_id=0, has_side_effects=True, vmem_limit_bytes=48 << 20
        ),
    )(
        latent.reshape(256, D),
        modulation,
        qkv_spatial.transpose(0, 2, 1),
        gcol,
        grow,
        wsh,
    )
    gcol, grow = gains(gain_temporal)
    result = pl.pallas_call(
        temporal_kernel,
        name="temporal",
        out_shape=jax.ShapeDtypeStruct((256, D), BF16),
        in_specs=[vmem] * 5 + [hbm],
        out_specs=vmem,
        scratch_shapes=[
            pltpu.VMEM((N_SEQ, 8, D), BF16),
            pltpu.VMEM((N_SEQ, 8, D), BF16),
            pltpu.VMEM((N_SEQ, 8, D), BF16),
            pltpu.VMEM((N_TP, HW, 256), BF16),
            pltpu.VMEM((N_TP, 27, 16, D), BF16),
            pltpu.VMEM((N_TP, 9, 16, D), BF16),
            pltpu.VMEM((N_TP, 36, 16, D), BF16),
            pltpu.VMEM((N_TP, 36, 16, D), BF16),
            pltpu.VMEM((256, D), F32),
            dma((N_SEQ,)),
            dma((N_SEQ,)),
            dma((N_SEQ,)),
            dma((N_SEQ,)),
            dma((4,)),
        ],
        compiler_params=pltpu.CompilerParams(
            collective_id=1, has_side_effects=True, vmem_limit_bytes=60 << 20
        ),
    )(nrm, mid, modulation, gcol, grow, g.reshape(N_TP, 128, 16, D))
    return result.reshape(latent.shape)


def solution(mesh):
    placed = (
        P(None, "seq", "tp", None),
        P(),
        P(None, None, "tp"),
        P(),
        P("tp", None),
        P(None, None, "tp"),
        P(),
        P("tp", None),
        P(None, "tp"),
        P("tp", None),
    )
    return jax.shard_map(
        body, mesh=mesh, in_specs=placed, out_specs=P(None, "seq", "tp", None), check_vma=False
    )
```

```python
import math

import jax
import jax.numpy as jnp
from jax import lax
from jax.experimental import pallas as pl
from jax.experimental.pallas import tpu as pltpu
from jax.sharding import PartitionSpec as P

D = 1152
H = 16
HD = 72
HW = 144
N_TP = 8
N_SEQ = 32
MESH = pl.DeviceIdType.MESH
EPS = 1e-06
SCALE = 1.0 / math.sqrt(HD)
F32 = jnp.float32
BF16 = jnp.bfloat16

ATT = 2
ROUNDS = 5


def layer_norm(values):
    average = jnp.mean(values, axis=-1, keepdims=True)
    centred = values - average
    variance = jnp.mean(centred * centred, axis=-1, keepdims=True)
    return centred * lax.rsqrt(variance + EPS)


def dot(left, right, left_dim=1, right_dim=0):
    return lax.dot_general(
        left, right, (((left_dim,), (right_dim,)), ((), ())), preferred_element_type=F32
    )


def head_norm_rows(values, gain):
    halves = []
    for head in range(2):
        part = values[head * HD : (head + 1) * HD]
        halves.append(part * lax.rsqrt(jnp.mean(part * part, axis=0, keepdims=True) + EPS))
    return jnp.concatenate(halves, axis=0) * gain


def head_norm_lanes(values, gain):
    first = lax.broadcasted_iota(jnp.int32, values.shape, 1) < HD
    square = values * values
    low = jnp.sum(jnp.where(first, square, 0.0), axis=-1, keepdims=True)
    high = jnp.sum(jnp.where(first, 0.0, square), axis=-1, keepdims=True)
    factor = jnp.where(
        first, lax.rsqrt(low * (1.0 / HD) + EPS), lax.rsqrt(high * (1.0 / HD) + EPS)
    )
    return values * factor * gain


def remote(src, dst, send_sem, recv_sem, seq, tp):
    return pltpu.make_async_remote_copy(
        src_ref=src,
        dst_ref=dst,
        send_sem=send_sem,
        recv_sem=recv_sem,
        device_id={"seq": seq, "tp": tp},
        device_id_type=MESH,
    )


def scope(name):
    return jax.named_scope(name)


def block_kernel(
    lat,
    mod,
    gains,
    wqkv,
    src_os,
    src_qkv,
    src_ot,
    src_1,
    src_2,
    result,
    xs,
    ks,
    qs,
    vs,
    ot,
    heads,
    ga,
    gm,
    mid,
    nrm,
    rows_in,
    rows_out,
    rows_back,
    tt,
    nm,
    total,
    part_out,
    part_in,
    ag_send,
    ag_recv,
    s1_send,
    s1_recv,
    own_sem,
    w_send,
    w_recv,
    d_send,
    d_recv,
    h_send,
    h_recv,
    f_send,
    f_recv,
    b_send,
    b_recv,
    m_send,
    m_recv,
):
    seq, me = lax.axis_index("seq"), lax.axis_index("tp")
    x, zh, y = seq // 8, lax.rem(seq // 4, 2), lax.rem(seq, 4)
    zl, c = me // 2, lax.rem(me, 2)
    sib = zl * 2 + (1 - c)
    unit = x * 4 + y

    def xy(dx, dy):
        return (lax.rem(x + dx + 4, 4) * 2 + zh) * 4 + lax.rem(y + dy + 4, 4)

    def zdev(dz):
        z = lax.rem(zh * 4 + zl + dz + 8, 8)
        return (x * 2 + z // 4) * 4 + y, lax.rem(z, 4) * 2 + c

    ring = (xy(1, 0), xy(-1, 0), xy(0, 1), xy(0, -1))
    peers = [(seq, lax.rem(me + i, N_TP)) for i in range(1, N_TP)]
    peers += [zdev(dz) for dz in (1, -1, 2, -2)]
    barrier = pltpu.get_barrier_semaphore()

    def signal(to_seq, to_tp):
        pl.semaphore_signal(
            barrier, inc=1, device_id={"seq": to_seq, "tp": to_tp}, device_id_type=MESH
        )

    for to_seq, to_tp in peers:
        signal(to_seq, to_tp)

    def signal_seq(i, _):
        signal(lax.rem(seq + i, N_SEQ), me)
        return 0

    lax.fori_loop(1, N_SEQ, signal_seq, 0)

    def spot(k, zs, xi, yi):
        return ga.at[zs, c, xi, yi, k] if k < ATT else gm.at[zs, xi, yi, k - ATT]

    def s1_copies(k, src):
        here = spot(k, zl, x, y)
        return [
            remote(src, here, s1_send.at[k, i], s1_recv.at[k, zl], *zdev(dz))
            for i, dz in enumerate((1, -1, 2 if k % 2 == 0 else -2))
        ]

    def s1_start(k):
        if k < ATT:
            tables = ((src_os, 0, 3), (src_qkv, 3, 12), (src_ot, 12, 16))
        else:
            tables = ((src_1, 0, 8), (src_2, 8, 16))
        for table, low, high in tables:

            @pl.when((unit >= low) & (unit < high))
            def _():
                at = jnp.clip(unit - low, 0, table.shape[0] - 1)
                src = table.at[at, k if k < ATT else k - ATT]
                pltpu.make_async_copy(src, spot(k, zl, x, y), own_sem.at[k]).start()
                for copy in s1_copies(k, src):
                    copy.start()

    def s1_wait(k):
        here = spot(k, zl, x, y)
        pltpu.make_async_copy(src_1.at[0, 0], here, own_sem.at[k]).wait()
        for i in range(1, 4):
            source = lax.rem(zl + i, 4)
            there = spot(k, source, x, y)
            remote(there, there, s1_send.at[k, 0], s1_recv.at[k, source], seq, sib).wait_recv()

    x_back, x_next = lax.rem(x + 3, 4), lax.rem(x + 1, 4)
    y_back, y_next = lax.rem(y + 3, 4), lax.rem(y + 1, 4)
    low, high = pl.ds(0, 2), pl.ds(2, 2)
    every = slice(None)

    def ring_copies(stage, k):
        if stage == 0:
            spots = [spot(k, low, x, y)] * 2 + [spot(k, high, x, y)] * 2
        elif stage == 1:
            spots = [
                spot(k, 0, x_back, y),
                spot(k, 1, x_next, y),
                spot(k, 2, x, y_back),
                spot(k, 3, x, y_next),
            ]
        elif stage == 2:
            spots = [spot(k, high, x, every)] * 2 + [spot(k, low, every, y)] * 2
        else:
            spots = [
                spot(k, 2, x_back, every),
                spot(k, 3, x_next, every),
                spot(k, 0, every, y_back),
                spot(k, 1, every, y_next),
            ]
        return [
            remote(there, there, w_send.at[stage, k, i], w_recv.at[stage, k, i], ring[i], me)
            for i, there in enumerate(spots)
        ]

    def ring_start(stage, k):
        for copy in ring_copies(stage, k):
            copy.start()

    def ring_wait(stage, k):
        for copy in ring_copies(stage, k):
            copy.wait_recv()

    def core_copy(k):
        there = ga.at[:, c, :, :, k]
        return remote(there, there, d_send.at[k], d_recv.at[k], seq, sib)

    def pump(step, k):
        with scope(f"pump_{step}_{k}"):
            if step == 0:
                s1_start(k)
            elif step == 1:
                s1_wait(k)
                ring_start(0, k)
            elif step <= 4:
                ring_wait(step - 2, k)
                ring_start(step - 1, k)
            elif step == 5:
                ring_wait(3, k)
                if k < ATT:
                    core_copy(k).start()
            else:
                core_copy(k).wait_recv()

    def ag_copy(slot, b, way):
        to = (jnp.minimum(zl + 1, 3) * 2 + c, jnp.maximum(zl - 1, 0) * 2 + c, sib)[way]
        there = xs.at[slot, b]
        return remote(there, there, ag_send.at[slot, b, way], ag_recv.at[slot, b], seq, to)

    def ag_step(distance, b, what):
        with scope(f"ag_{distance}_{b}_{what}"):
            ag_now(distance, b, what)

    def ag_now(distance, b, what):
        for way in range(2):
            origin = zl - distance if way == 0 else zl + distance
            there = (zl >= distance) if way == 0 else (zl + distance <= 3)
            more = (zl < 3) if way == 0 else (zl > 0)
            if distance == 0:
                there = more
            slot = origin * 2 + c

            @pl.when(there)
            def _():
                if what == 0 and distance > 0:
                    ag_copy(slot, b, 2).wait_recv()
                if distance == 0:
                    copy = ag_copy(slot, b, way)
                    copy.start() if what == 0 else copy.wait_send()
                else:

                    @pl.when(more)
                    def _():
                        copy = ag_copy(slot, b, way)
                        copy.start() if what == 0 else copy.wait_send()

                    copy = ag_copy(slot, b, 2)
                    copy.start() if what == 0 else copy.wait_send()

        if distance == 0:
            copy = ag_copy(me, b, 2)
            copy.start() if what == 0 else copy.wait_send()

    first_col = lax.broadcasted_iota(jnp.int32, (HW, HW), 0) == lax.broadcasted_iota(
        jnp.int32, (HW, HW), 1
    )

    def gain_column(i):
        return jnp.sum(jnp.where(first_col, gains[i : i + 1], 0.0), axis=1, keepdims=True)

    def project(z):
        with scope("project"):
            rows = xs[pl.ds(z * 2, 2)].reshape(512, D)
            queries = head_norm_rows(dot(wqkv[0], rows, 1, 1), gain_column(0)).astype(BF16)
            values = dot(wqkv[2], rows, 1, 1).astype(BF16)
            keys = head_norm_lanes(dot(rows, wqkv[1], 1, 1), gains[1:2]).astype(BF16)
            for core in range(2):
                for b in range(2):
                    at = (core * 2 + b) * 128
                    qs[b, z * 2 + core] = queries[:, at : at + 128]
                    there = pl.ds(pl.multiple_of((z * 2 + core) * 128, 128), 128)
                    vs[b, :, there] = values[:, at : at + 128]
                    ks[b, z * 2 + core] = keys[at : at + 128]

    def head_copy(b, to):
        return remote(
            ot.at[b, to], heads.at[b, me], h_send.at[b, to], h_recv.at[b, me], seq, to
        )

    def attend(b):
        with scope(f"attend_{b}"):
            attend_now(b)

    def attend_now(b):
        keys = ks[b].reshape(N_TP * 128, HW)
        values = vs[b]

        def block(i, _):
            to = lax.rem(me + 1 + i, N_TP)
            query = qs[b, to].astype(F32)
            zero = jnp.zeros((HD, 128), F32)
            pair = jnp.concatenate(
                [
                    jnp.concatenate([query[:HD], zero], axis=0),
                    jnp.concatenate([zero, query[HD:]], axis=0),
                ],
                axis=1,
            ).astype(BF16)
            weights = jnp.exp(dot(keys, pair) * SCALE)
            norm = jnp.sum(weights, axis=0, keepdims=True)
            mixed = dot(values, weights.astype(BF16)) / norm
            out = jnp.concatenate([mixed[:HD, :128], mixed[HD:, 128:]], axis=0).astype(BF16)

            @pl.when(to != me)
            def _():
                ot[b, to] = out
                head_copy(b, to).start()

            @pl.when(to == me)
            def _():
                heads[b, me] = out

            return 0

        lax.fori_loop(0, N_TP, block, 0)

    def send_rows(source, target, send, recv, b):
        def start(i, _):
            to = lax.rem(seq + i, N_SEQ)

            @pl.when((to // 16 == b) | (b < 0))
            def _():
                remote(source.at[to], target.at[seq], send.at[to], recv.at[seq], to, me).start()

            return 0

        lax.fori_loop(1, N_SEQ, start, 0)

    def take_rows(source, target, send, recv):
        target[seq] = source[seq]

        def finish(i, _):
            sender = lax.rem(seq + i, N_SEQ)
            there = target.at[sender]
            remote(there, there, send.at[sender], recv.at[sender], sender, me).wait_recv()
            return 0

        lax.fori_loop(1, N_SEQ, finish, 0)

    def drain(source, send, recv):
        def finish(i, _):
            to = lax.rem(seq + i, N_SEQ)
            there = source.at[to]
            remote(there, there, send.at[to], recv.at[to], to, me).wait_send()
            return 0

        lax.fori_loop(1, N_SEQ, finish, 0)

    def finish(b):
        with scope(f"finish_{b}"):
            for i in range(1, N_TP):
                source = lax.rem(me + i, N_TP)
                there = heads.at[b, source]
                remote(
                    there, there, h_send.at[b, source], h_recv.at[b, source], seq, source
                ).wait_recv()
            mixed = heads[b].reshape(D, 128).T
            out = dot(mixed, ga[:, :, 0, 0:3].reshape(D, D)).astype(BF16).astype(F32)
            rows = pl.ds(b * 128, 128)
            late = lat[rows].astype(F32) + mod[b, 2:3] * out
            mid[rows] = late
            normed = layer_norm(late) * (1.0 + mod[b, 4:5]) + mod[b, 3:4]
            nrm[pl.ds(b * 16, 16)] = normed.reshape(16, 8, D).astype(BF16)
            send_rows(nrm, rows_in, f_send, f_recv, b)

    def att_rows(z, core, first):
        return jnp.concatenate(
            [ga[z, core, u // 4, u % 4].reshape(48, D) for u in range(first, first + 3)], axis=0
        )

    def temporal():
        rows = rows_in[...].astype(F32).reshape(256, D).astype(BF16)
        same = lax.rem(lax.broadcasted_iota(jnp.int32, (256, 256), 0), 8) == lax.rem(
            lax.broadcasted_iota(jnp.int32, (256, 256), 1), 8
        )
        column = gain_column(2)
        zero = jnp.zeros((HD, 256), F32)

        def pair_of_heads(t, _):
            z, core = t // 2, lax.rem(t, 2)
            queries = head_norm_rows(dot(att_rows(z, core, 3), rows, 1, 1), column)
            keys = head_norm_lanes(dot(rows, att_rows(z, core, 6), 1, 1), gains[3:4]).astype(BF16)
            values = dot(att_rows(z, core, 9), rows, 1, 1).astype(BF16)
            parts = []
            for head in range(2):
                kept = queries[head * HD : (head + 1) * HD]
                kept = jnp.concatenate([kept, zero] if head == 0 else [zero, kept], axis=0)
                probs = jnp.where(same, jnp.exp(dot(keys, kept.astype(BF16)) * SCALE), 0.0)
                norm = jnp.sum(probs, axis=0, keepdims=True)
                mixed = dot(values, probs.astype(BF16)) / norm
                parts.append(mixed[head * HD : (head + 1) * HD])
            tt[t] = jnp.concatenate(parts, axis=0).astype(BF16)
            return 0

        lax.fori_loop(0, N_TP, pair_of_heads, 0)
        out = dot(tt[...].reshape(D, 256).T, ga[:, :, 3, 0:3].reshape(D, D))
        rows_out[...] = out.reshape(N_SEQ, 8, D).astype(BF16)

    def half_copy():
        return remote(nm.at[c], nm.at[c], m_send.at[0], m_recv.at[0], seq, sib)

    def part_copy():
        return remote(part_out, part_in, m_send.at[1], m_recv.at[1], seq, sib)

    def mlp_entry():
        back = rows_back[...].astype(F32).reshape(256, D)
        for b in range(2):
            rows = pl.ds(b * 128, 128)
            late = mid[rows] + mod[b, 5:6] * back[b * 128 : (b + 1) * 128]
            mid[rows] = late
            normed = layer_norm(late) * (1.0 + mod[b, 7:8]) + mod[b, 6:7]
            nm[c, rows] = normed.astype(BF16)

    def mlp_round(k, which):
        u = dot(nm[which], gm[:, 0:2, :, k].reshape(768, D), 1, 1)
        h = 0.5 * u * (1.0 + jnp.tanh(math.sqrt(2.0 / math.pi) * (u + 0.044715 * (u * u * u))))
        product = dot(h.astype(BF16), gm[:, 2:4, :, k].reshape(768, D))
        return product if k == 0 else total[which] + product

    for b in range(2):
        rows = lat[pl.ds(b * 128, 128)].astype(F32)
        xs[me, b] = (layer_norm(rows) * (1.0 + mod[b, 1:2]) + mod[b, 0:1]).astype(BF16)
    with scope("greet"):
        pl.semaphore_wait(barrier, len(peers) + N_SEQ - 1)
    pump(0, 0)
    ag_step(0, 0, 0)
    ag_step(0, 1, 0)
    pump(0, 1)
    for b in range(2):
        ag_copy(sib, b, 2).wait_recv()
    project(zl)
    pump(1, 0)
    ag_step(1, 0, 0)
    pump(1, 1)
    pump(2, 0)
    ag_step(1, 1, 0)
    pump(2, 1)
    pump(3, 0)
    ag_step(2, 0, 0)
    pump(3, 1)
    pump(0, 2)
    ag_step(2, 1, 0)
    pump(1, 2)
    ag_step(3, 0, 0)
    pump(4, 0)
    ag_step(3, 1, 0)
    pump(0, 3)
    for distance in range(1, 4):
        for b in range(2):
            other = lax.rem(zl + distance, 4) * 2 + (1 - c)
            ag_copy(other, b, 2).wait_recv()
    for i in range(1, 4):
        project(lax.rem(zl + i, 4))
    pump(2, 2)
    attend(0)
    pump(4, 1)
    pump(5, 0)
    pump(0, 4)
    attend(1)
    pump(1, 3)
    pump(3, 2)
    pump(5, 1)
    pump(6, 0)
    pump(6, 1)
    finish(0)
    finish(1)
    pump(2, 3)
    pump(1, 4)
    with scope("take_1"):
        take_rows(nrm, rows_in, f_send, f_recv)
    pump(4, 2)
    pump(3, 3)
    with scope("temporal"):
        temporal()
    send_rows(rows_out, rows_back, b_send, b_recv, -1)
    pump(2, 4)
    pump(4, 3)
    pump(3, 4)
    with scope("take_2"):
        take_rows(rows_out, rows_back, b_send, b_recv)
    with scope("entry"):
        mlp_entry()
        half_copy().start()
    pump(5, 2)
    with scope("mlp"):
        total[c] = mlp_round(0, c)
        half_copy().wait_recv()
        total[1 - c] = mlp_round(0, 1 - c)
    pump(4, 4)
    pump(5, 3)
    with scope("mlp"):
        total[c] = mlp_round(1, c)
        total[1 - c] = mlp_round(1, 1 - c)
    pump(5, 4)
    with scope("mlp"):
        part_out[...] = mlp_round(2, 1 - c).astype(BF16)
        part_copy().start()
        total[c] = mlp_round(2, c)
    with scope("last"):
        part_copy().wait_recv()
        for b in range(2):
            rows = pl.ds(b * 128, 128)
            out = (total[c, rows] + part_in[rows].astype(F32)).astype(BF16).astype(F32)
            result[rows] = (mid[rows] + mod[b, 8:9] * out).astype(BF16)

    with scope("drain"):
        half_copy().wait_send()
        part_copy().wait_send()
        drain(nrm, f_send, f_recv)
        drain(rows_out, b_send, b_recv)
        for b in range(2):
            for distance in range(4):
                ag_step(distance, b, 1)
            for i in range(1, N_TP):
                head_copy(b, lax.rem(me + i, N_TP)).wait_send()
        for k in range(ROUNDS):
            for copy in s1_copies(k, src_1.at[0, 0]):
                copy.wait_send()
            for stage in range(4):
                for copy in ring_copies(stage, k):
                    copy.wait_send()
            if k < ATT:
                core_copy(k).wait_send()


def body(
    latent,
    modulation,
    qkv_spatial,
    gain_spatial,
    out_spatial,
    qkv_temporal,
    gain_temporal,
    out_temporal,
    fc_in,
    fc_out,
):
    gains = jnp.concatenate([gain_spatial, gain_temporal], axis=0)
    gains = jnp.concatenate([gains, gains], axis=1)
    vmem = pl.BlockSpec(memory_space=pltpu.VMEM)
    hbm = pl.BlockSpec(memory_space=pl.ANY)
    dma = pltpu.SemaphoreType.DMA
    result = pl.pallas_call(
        block_kernel,
        name="block",
        out_shape=jax.ShapeDtypeStruct((256, D), BF16),
        in_specs=[vmem] * 4 + [hbm] * 5,
        out_specs=vmem,
        scratch_shapes=[
            pltpu.VMEM((N_TP, 2, 128, D), BF16),
            pltpu.VMEM((2, N_TP, 128, HW), BF16),
            pltpu.VMEM((2, N_TP, HW, 128), BF16),
            pltpu.VMEM((2, HW, 1024), BF16),
            pltpu.VMEM((2, N_TP, HW, 128), BF16),
            pltpu.VMEM((2, N_TP, HW, 128), BF16),
            pltpu.VMEM((4, 2, 4, 4, ATT, 24, D), BF16),
            pltpu.VMEM((4, 4, 4, ROUNDS - ATT, 24, D), BF16),
            pltpu.VMEM((256, D), F32),
            pltpu.VMEM((N_SEQ, 8, D), BF16),
            pltpu.VMEM((N_SEQ, 8, D), BF16),
            pltpu.VMEM((N_SEQ, 8, D), BF16),
            pltpu.VMEM((N_SEQ, 8, D), BF16),
            pltpu.VMEM((N_TP, HW, 256), BF16),
            pltpu.VMEM((2, 256, D), BF16),
            pltpu.VMEM((2, 256, D), F32),
            pltpu.VMEM((256, D), BF16),
            pltpu.VMEM((256, D), BF16),
            dma((N_TP, 2, 3)),
            dma((N_TP, 2)),
            dma((ROUNDS, 3)),
            dma((ROUNDS, 4)),
            dma((ROUNDS,)),
            dma((4, ROUNDS, 4)),
            dma((4, ROUNDS, 4)),
            dma((ATT,)),
            dma((ATT,)),
            dma((2, N_TP)),
            dma((2, N_TP)),
            dma((N_SEQ,)),
            dma((N_SEQ,)),
            dma((N_SEQ,)),
            dma((N_SEQ,)),
            dma((2,)),
            dma((2,)),
        ],
        compiler_params=pltpu.CompilerParams(
            collective_id=0, has_side_effects=True, vmem_limit_bytes=60 << 20
        ),
    )(
        latent.reshape(256, D),
        modulation,
        gains,
        qkv_spatial.transpose(0, 2, 1),
        out_spatial.reshape(3, ATT, 24, D),
        qkv_temporal.transpose(0, 2, 1).reshape(9, ATT, 24, D),
        out_temporal.reshape(3, ATT, 24, D),
        fc_in.T.reshape(8, ROUNDS - ATT, 24, D),
        fc_out.reshape(8, ROUNDS - ATT, 24, D),
    )
    return result.reshape(latent.shape)


def solution(mesh):
    placed = (
        P(None, "seq", "tp", None),
        P(),
        P(None, None, "tp"),
        P(),
        P("tp", None),
        P(None, None, "tp"),
        P(),
        P("tp", None),
        P(None, "tp"),
        P("tp", None),
    )
    return jax.shard_map(
        body, mesh=mesh, in_specs=placed, out_specs=P(None, "seq", "tp", None), check_vma=False
    )
```

```python
import math

import jax
import jax.numpy as jnp
from jax import lax
from jax.experimental import pallas as pl
from jax.experimental.pallas import tpu as pltpu
from jax.sharding import PartitionSpec as P

D = 1152
H = 16
HD = 72
HW = 144
N_TP = 8
N_SEQ = 32
MESH = pl.DeviceIdType.MESH
EPS = 1e-06
SCALE = 1.0 / math.sqrt(HD)
F32 = jnp.float32
BF16 = jnp.bfloat16

ATT = 2
ROUNDS = 5


def layer_norm(values):
    average = jnp.mean(values, axis=-1, keepdims=True)
    centred = values - average
    variance = jnp.mean(centred * centred, axis=-1, keepdims=True)
    return centred * lax.rsqrt(variance + EPS)


def dot(left, right, left_dim=1, right_dim=0):
    return lax.dot_general(
        left, right, (((left_dim,), (right_dim,)), ((), ())), preferred_element_type=F32
    )


def head_norm_rows(values, gain):
    halves = []
    for head in range(2):
        part = values[head * HD : (head + 1) * HD]
        halves.append(part * lax.rsqrt(jnp.mean(part * part, axis=0, keepdims=True) + EPS))
    return jnp.concatenate(halves, axis=0) * gain


def head_norm_lanes(values, gain):
    first = lax.broadcasted_iota(jnp.int32, values.shape, 1) < HD
    square = values * values
    low = jnp.sum(jnp.where(first, square, 0.0), axis=-1, keepdims=True)
    high = jnp.sum(jnp.where(first, 0.0, square), axis=-1, keepdims=True)
    factor = jnp.where(
        first, lax.rsqrt(low * (1.0 / HD) + EPS), lax.rsqrt(high * (1.0 / HD) + EPS)
    )
    return values * factor * gain


def remote(src, dst, send_sem, recv_sem, seq, tp):
    return pltpu.make_async_remote_copy(
        src_ref=src,
        dst_ref=dst,
        send_sem=send_sem,
        recv_sem=recv_sem,
        device_id={"seq": seq, "tp": tp},
        device_id_type=MESH,
    )


def scope(name):
    return jax.named_scope(name)


def block_kernel(
    lat,
    mod,
    gain_s,
    gain_t,
    wqkv,
    src_os,
    src_qkv,
    src_ot,
    src_1,
    src_2,
    result,
    xs,
    ks,
    qs,
    vs,
    ot,
    heads,
    ga,
    gm,
    mid,
    nrm,
    rows_in,
    rows_out,
    rows_back,
    tt,
    nm,
    total,
    part_out,
    part_in,
    ag_send,
    ag_recv,
    s1_send,
    s1_recv,
    own_sem,
    w_send,
    w_recv,
    d_send,
    d_recv,
    h_send,
    h_recv,
    x_sem,
    m_send,
    m_recv,
):
    seq, me = lax.axis_index("seq"), lax.axis_index("tp")
    x, zh, y = seq // 8, lax.rem(seq // 4, 2), lax.rem(seq, 4)
    zl, c = me // 2, lax.rem(me, 2)
    sib = zl * 2 + (1 - c)
    unit = x * 4 + y

    def xy(dx, dy):
        return (lax.rem(x + dx + 4, 4) * 2 + zh) * 4 + lax.rem(y + dy + 4, 4)

    def zdev(dz):
        z = lax.rem(zh * 4 + zl + dz + 8, 8)
        return (x * 2 + z // 4) * 4 + y, lax.rem(z, 4) * 2 + c

    ring = (xy(1, 0), xy(-1, 0), xy(0, 1), xy(0, -1))
    peers = [(seq, lax.rem(me + i, N_TP)) for i in range(1, N_TP)]
    peers += [zdev(dz) for dz in (1, -1, 2, -2)]
    barrier = pltpu.get_barrier_semaphore()

    def signal(to_seq, to_tp):
        pl.semaphore_signal(
            barrier, inc=1, device_id={"seq": to_seq, "tp": to_tp}, device_id_type=MESH
        )

    for to_seq, to_tp in peers:
        signal(to_seq, to_tp)

    def signal_seq(i, _):
        signal(lax.rem(seq + i, N_SEQ), me)
        return 0

    lax.fori_loop(1, N_SEQ, signal_seq, 0)

    def bytes_of(ref, sem):
        pltpu.make_async_copy(ref, ref, sem).wait()

    def spot(k, zs, xi, yi):
        return ga.at[zs, c, xi, yi, k] if k < ATT else gm.at[zs, xi, yi, k - ATT]

    def s1_copies(k, src):
        here = spot(k, zl, x, y)
        far = (zl // 2) * 4 - 2
        return [
            remote(src, here, s1_send.at[k], s1_recv.at[k], *zdev(dz))
            for dz in (1, -1, far)
        ]

    def s1_start(k):
        if k < ATT:
            tables = ((src_os, 0, 3), (src_qkv, 3, 12), (src_ot, 12, 16))
        else:
            tables = ((src_1, 0, 8), (src_2, 8, 16))
        for table, low, high in tables:

            @pl.when((unit >= low) & (unit < high))
            def _():
                at = jnp.clip(unit - low, 0, table.shape[0] - 1)
                src = table.at[at, k if k < ATT else k - ATT]
                pltpu.make_async_copy(src, spot(k, zl, x, y), own_sem.at[k]).start()
                for copy in s1_copies(k, src):
                    copy.start()

    def s1_wait(k):
        here = spot(k, zl, x, y)
        pltpu.make_async_copy(src_1.at[0, 0], here, own_sem.at[k]).wait()
        bytes_of(gm.at[0, 0, 0], s1_recv.at[k])

    x_back, x_next = lax.rem(x + 3, 4), lax.rem(x + 1, 4)
    y_back, y_next = lax.rem(y + 3, 4), lax.rem(y + 1, 4)
    low, high = pl.ds(0, 2), pl.ds(2, 2)
    every = slice(None)

    def ring_copies(stage, k):
        if stage == 0:
            spots = [spot(k, low, x, y)] * 2 + [spot(k, high, x, y)] * 2
        elif stage == 1:
            spots = [
                spot(k, 0, x_back, y),
                spot(k, 1, x_next, y),
                spot(k, 2, x, y_back),
                spot(k, 3, x, y_next),
            ]
        elif stage == 2:
            spots = [spot(k, high, x, every)] * 2 + [spot(k, low, every, y)] * 2
        else:
            spots = [
                spot(k, 2, x_back, every),
                spot(k, 3, x_next, every),
                spot(k, 0, every, y_back),
                spot(k, 1, every, y_next),
            ]
        return [
            remote(there, there, w_send.at[stage, k], w_recv.at[stage, k], ring[i], me)
            for i, there in enumerate(spots)
        ]

    def ring_start(stage, k):
        for copy in ring_copies(stage, k):
            copy.start()

    def ring_wait(stage, k):
        bytes_of(ring_bytes(stage), w_recv.at[stage, k])

    def ring_bytes(stage):
        return (gm.at[:, 0, 0:2, 0], gm.at[:, 0, 0, 0], gm.at[:, 0:2, :, 0], gm.at[:, 0, :, 0])[
            stage
        ]

    def core_copy(k):
        there = ga.at[:, c, :, :, k]
        return remote(there, there, d_send.at[k], d_recv.at[k], seq, sib)

    def pump(step, k):
        with scope(f"pump_{step}_{k}"):
            if step == 0:
                s1_start(k)
            elif step == 1:
                s1_wait(k)
                ring_start(0, k)
            elif step <= 4:
                ring_wait(step - 2, k)
                ring_start(step - 1, k)
            elif step == 5:
                ring_wait(3, k)
                if k < ATT:
                    core_copy(k).start()
            else:
                core_copy(k).wait_recv()

    def ag_copy(slot, b, way):
        to = (jnp.minimum(zl + 1, 3) * 2 + c, jnp.maximum(zl - 1, 0) * 2 + c, sib)[way]
        there = xs.at[slot, b]
        return remote(there, there, ag_send.at[way], ag_recv.at[slot, b], seq, to)

    def ag_step(distance, b):
        with scope(f"ag_{distance}_{b}"):
            ag_now(distance, b)

    def ag_now(distance, b):
        for way in range(2):
            origin = zl - distance if way == 0 else zl + distance
            there = (zl >= distance) if way == 0 else (zl + distance <= 3)
            more = (zl < 3) if way == 0 else (zl > 0)
            slot = origin * 2 + c

            @pl.when(there)
            def _():
                if distance > 0:
                    ag_copy(slot, b, 2).wait_recv()

                @pl.when(more)
                def _():
                    ag_copy(slot, b, way).start()

                if distance > 0 or way == 0:
                    ag_copy(slot, b, 2).start()

    def ag_drain():
        bytes_of(xs.at[0:4], ag_send.at[2])
        for z in range(4):

            @pl.when(zl == z)
            def _():
                if z < 3:
                    bytes_of(xs.at[0 : z + 1], ag_send.at[0])
                if z > 0:
                    bytes_of(xs.at[0 : 4 - z], ag_send.at[1])

    def diagonal(n):
        return lax.broadcasted_iota(jnp.int32, (n, n), 0) == lax.broadcasted_iota(
            jnp.int32, (n, n), 1
        )

    def gain_column(gains, i):
        column = jnp.where(diagonal(HD), gains[i : i + 1], 0.0)
        column = jnp.sum(column, axis=1, keepdims=True)
        return jnp.concatenate([column, column], axis=0)

    def gain_row(gains, i):
        return jnp.sum(
            jnp.where(diagonal(HW), gain_column(gains, i), 0.0), axis=0, keepdims=True
        )

    query_gain, key_gain = gain_column(gain_s, 0), gain_row(gain_s, 1)

    def project(z, b):
        with scope("project"):
            rows = xs[pl.ds(z * 2, 2), b].reshape(256, D)
            queries = head_norm_rows(dot(wqkv[0], rows, 1, 1), query_gain).astype(BF16)
            values = dot(wqkv[2], rows, 1, 1).astype(BF16)
            keys = head_norm_lanes(dot(rows, wqkv[1], 1, 1), key_gain).astype(BF16)
            for core in range(2):
                at = core * 128
                qs[b, z * 2 + core] = queries[:, at : at + 128]
                there = pl.ds(pl.multiple_of((z * 2 + core) * 128, 128), 128)
                vs[b, :, there] = values[:, at : at + 128]
                ks[b, z * 2 + core] = keys[at : at + 128]

    def take_core(z, b):
        ag_copy(z * 2 + (1 - c), b, 2).wait_recv()

    def head_copy(b, to):
        return remote(
            ot.at[b, to], heads.at[b, me], h_send.at[b], h_recv.at[b], seq, to
        )

    def attend(b):
        with scope(f"attend_{b}"):
            attend_now(b)

    def attend_now(b):
        keys = ks[b].reshape(N_TP * 128, HW)
        values = vs[b]

        def block(i, _):
            to = lax.rem(me + 1 + i, N_TP)
            query = qs[b, to].astype(F32)
            zero = jnp.zeros((HD, 128), F32)
            pair = jnp.concatenate(
                [
                    jnp.concatenate([query[:HD], zero], axis=0),
                    jnp.concatenate([zero, query[HD:]], axis=0),
                ],
                axis=1,
            ).astype(BF16)
            weights = jnp.exp(dot(keys, pair) * SCALE)
            norm = jnp.sum(weights, axis=0, keepdims=True)
            mixed = dot(values, weights.astype(BF16)) / norm
            out = jnp.concatenate([mixed[:HD, :128], mixed[HD:, 128:]], axis=0).astype(BF16)

            @pl.when(to != me)
            def _():
                ot[b, to] = out
                head_copy(b, to).start()

            @pl.when(to == me)
            def _():
                heads[b, me] = out

            return 0

        lax.fori_loop(0, N_TP, block, 0)

    def send_rows(source, target, send, recv, b):
        def start(i, _):
            to = lax.rem(seq + i, N_SEQ)

            @pl.when((to // 16 == b) | (b < 0))
            def _():
                remote(source.at[to], target.at[seq], send, recv, to, me).start()

            return 0

        lax.fori_loop(1, N_SEQ, start, 0)

    def take_rows(source, target, recv):
        target[seq] = source[seq]
        bytes_of(target.at[0:31], recv)

    def finish(b):
        with scope(f"finish_{b}"):
            bytes_of(heads.at[b, 0:7], h_recv.at[b])
            mixed = heads[b].reshape(D, 128).T
            out = dot(mixed, ga[:, :, 0, 0:3].reshape(D, D)).astype(BF16).astype(F32)
            rows = pl.ds(b * 128, 128)
            late = lat[rows].astype(F32) + mod[2, b : b + 1] * out
            mid[rows] = late
            normed = layer_norm(late) * (1.0 + mod[4, b : b + 1]) + mod[3, b : b + 1]
            nrm[pl.ds(b * 16, 16)] = normed.reshape(16, 8, D).astype(BF16)
            send_rows(nrm, rows_in, x_sem.at[0], x_sem.at[1], b)

    def att_rows(z, core, first):
        return jnp.concatenate(
            [ga[z, core, u // 4, u % 4].reshape(48, D) for u in range(first, first + 3)], axis=0
        )

    def temporal(half):
        rows = rows_in[...].astype(F32).reshape(256, D).astype(BF16)
        same = lax.rem(lax.broadcasted_iota(jnp.int32, (256, 256), 0), 8) == lax.rem(
            lax.broadcasted_iota(jnp.int32, (256, 256), 1), 8
        )
        column, row = gain_column(gain_t, 0), gain_row(gain_t, 1)
        zero = jnp.zeros((HD, 256), F32)

        def pair_of_heads(t, _):
            z, core = t // 2, lax.rem(t, 2)
            queries = head_norm_rows(dot(att_rows(z, core, 3), rows, 1, 1), column)
            keys = head_norm_lanes(dot(rows, att_rows(z, core, 6), 1, 1), row).astype(BF16)
            values = dot(att_rows(z, core, 9), rows, 1, 1).astype(BF16)
            parts = []
            for head in range(2):
                kept = queries[head * HD : (head + 1) * HD]
                kept = jnp.concatenate([kept, zero] if head == 0 else [zero, kept], axis=0)
                probs = jnp.where(same, jnp.exp(dot(keys, kept.astype(BF16)) * SCALE), 0.0)
                norm = jnp.sum(probs, axis=0, keepdims=True)
                mixed = dot(values, probs.astype(BF16)) / norm
                parts.append(mixed[head * HD : (head + 1) * HD])
            tt[t] = jnp.concatenate(parts, axis=0).astype(BF16)
            return 0

        lax.fori_loop(half * 4, half * 4 + 4, pair_of_heads, 0)
        if half == 0:
            return
        out = dot(tt[...].reshape(D, 256).T, ga[:, :, 3, 0:3].reshape(D, D))
        rows_out[...] = out.reshape(N_SEQ, 8, D).astype(BF16)

    def half_copy():
        return remote(nm.at[c], nm.at[c], m_send.at[0], m_recv.at[0], seq, sib)

    def part_copy():
        return remote(part_out, part_in, m_send.at[1], m_recv.at[1], seq, sib)

    def mlp_entry():
        back = rows_back[...].astype(F32).reshape(256, D)
        for b in range(2):
            rows = pl.ds(b * 128, 128)
            late = mid[rows] + mod[5, b : b + 1] * back[b * 128 : (b + 1) * 128]
            mid[rows] = late
            normed = layer_norm(late) * (1.0 + mod[7, b : b + 1]) + mod[6, b : b + 1]
            nm[c, rows] = normed.astype(BF16)

    def mlp_round(k, which):
        u = dot(nm[which], gm[:, 0:2, :, k].reshape(768, D), 1, 1)
        h = 0.5 * u * (1.0 + jnp.tanh(math.sqrt(2.0 / math.pi) * (u + 0.044715 * (u * u * u))))
        product = dot(h.astype(BF16), gm[:, 2:4, :, k].reshape(768, D))
        return product if k == 0 else total[which] + product

    for b in range(2):
        rows = lat[pl.ds(b * 128, 128)].astype(F32)
        xs[me, b] = (layer_norm(rows) * (1.0 + mod[1, b : b + 1]) + mod[0, b : b + 1]).astype(BF16)
    with scope("greet"):
        pl.semaphore_wait(barrier, len(peers) + N_SEQ - 1)
    near = zl + 1 - 2 * lax.rem(zl, 2)
    middle = 2 - zl // 2
    far = 3 - 3 * (zl // 2)
    pump(0, 0)
    pump(0, 1)
    ag_step(0, 0)
    ag_step(0, 1)
    for b in range(2):
        take_core(zl, b)
        project(zl, b)
    pump(1, 0)
    pump(1, 1)
    pump(2, 0)
    pump(2, 1)
    pump(3, 0)
    ag_step(1, 0)
    pump(3, 1)
    take_core(near, 0)
    project(near, 0)
    ag_step(1, 1)
    take_core(near, 1)
    project(near, 1)
    pump(0, 2)
    ag_step(2, 0)
    take_core(middle, 0)
    project(middle, 0)
    ag_step(2, 1)
    take_core(middle, 1)
    project(middle, 1)
    pump(4, 0)
    pump(1, 2)
    pump(0, 3)
    ag_step(3, 0)
    take_core(far, 0)
    project(far, 0)
    pump(4, 1)
    attend(0)
    pump(2, 2)
    pump(5, 0)
    pump(1, 3)
    ag_step(3, 1)
    take_core(far, 1)
    project(far, 1)
    pump(3, 2)
    pump(0, 4)
    attend(1)
    pump(5, 1)
    pump(2, 3)
    pump(6, 0)
    pump(6, 1)
    finish(0)
    finish(1)
    pump(3, 3)
    pump(1, 4)
    pump(4, 2)
    with scope("take_1"):
        take_rows(nrm, rows_in, x_sem.at[1])
    with scope("temporal"):
        temporal(0)
    pump(2, 4)
    with scope("temporal"):
        temporal(1)
    send_rows(rows_out, rows_back, x_sem.at[2], x_sem.at[3], -1)
    pump(4, 3)
    pump(3, 4)
    pump(5, 2)
    with scope("take_2"):
        take_rows(rows_out, rows_back, x_sem.at[3])
    with scope("entry"):
        mlp_entry()
        half_copy().start()
    with scope("mlp"):
        total[c] = mlp_round(0, c)
        half_copy().wait_recv()
        total[1 - c] = mlp_round(0, 1 - c)
    pump(5, 3)
    pump(4, 4)
    with scope("mlp"):
        total[c] = mlp_round(1, c)
        total[1 - c] = mlp_round(1, 1 - c)
    pump(5, 4)
    with scope("mlp"):
        part_out[...] = mlp_round(2, 1 - c).astype(BF16)
        part_copy().start()
        total[c] = mlp_round(2, c)
    with scope("last"):
        part_copy().wait_recv()
        for b in range(2):
            rows = pl.ds(b * 128, 128)
            out = (total[c, rows] + part_in[rows].astype(F32)).astype(BF16).astype(F32)
            result[rows] = (mid[rows] + mod[8, b : b + 1] * out).astype(BF16)

    with scope("drain"):
        half_copy().wait_send()
        part_copy().wait_send()
        bytes_of(nrm.at[0:31], x_sem.at[0])
        bytes_of(rows_out.at[0:31], x_sem.at[2])
        ag_drain()
        for b in range(2):
            bytes_of(ot.at[b, 0:7], h_send.at[b])
        for k in range(ROUNDS):
            bytes_of(gm.at[0, 0, 0], s1_send.at[k])
            for stage in range(4):
                bytes_of(ring_bytes(stage), w_send.at[stage, k])
            if k < ATT:
                core_copy(k).wait_send()


def body(
    latent,
    modulation,
    qkv_spatial,
    gain_spatial,
    out_spatial,
    qkv_temporal,
    gain_temporal,
    out_temporal,
    fc_in,
    fc_out,
):
    vmem = pl.BlockSpec(memory_space=pltpu.VMEM)
    hbm = pl.BlockSpec(memory_space=pl.ANY)
    dma = pltpu.SemaphoreType.DMA
    result = pl.pallas_call(
        block_kernel,
        name="block",
        out_shape=jax.ShapeDtypeStruct((256, D), BF16),
        in_specs=[vmem] * 5 + [hbm] * 5,
        out_specs=vmem,
        scratch_shapes=[
            pltpu.VMEM((N_TP, 2, 128, D), BF16),
            pltpu.VMEM((2, N_TP, 128, HW), BF16),
            pltpu.VMEM((2, N_TP, HW, 128), BF16),
            pltpu.VMEM((2, HW, 1024), BF16),
            pltpu.VMEM((2, N_TP, HW, 128), BF16),
            pltpu.VMEM((2, N_TP, HW, 128), BF16),
            pltpu.VMEM((4, 2, 4, 4, ATT, 24, D), BF16),
            pltpu.VMEM((4, 4, 4, ROUNDS - ATT, 24, D), BF16),
            pltpu.VMEM((256, D), F32),
            pltpu.VMEM((N_SEQ, 8, D), BF16),
            pltpu.VMEM((N_SEQ, 8, D), BF16),
            pltpu.VMEM((N_SEQ, 8, D), BF16),
            pltpu.VMEM((N_SEQ, 8, D), BF16),
            pltpu.VMEM((N_TP, HW, 256), BF16),
            pltpu.VMEM((2, 256, D), BF16),
            pltpu.VMEM((2, 256, D), F32),
            pltpu.VMEM((256, D), BF16),
            pltpu.VMEM((256, D), BF16),
            dma((3,)),
            dma((N_TP, 2)),
            dma((ROUNDS,)),
            dma((ROUNDS,)),
            dma((ROUNDS,)),
            dma((4, ROUNDS)),
            dma((4, ROUNDS)),
            dma((ATT,)),
            dma((ATT,)),
            dma((2,)),
            dma((2,)),
            dma((4,)),
            dma((2,)),
            dma((2,)),
        ],
        compiler_params=pltpu.CompilerParams(
            collective_id=0, has_side_effects=True, vmem_limit_bytes=60 << 20
        ),
    )(
        latent.reshape(256, D),
        modulation.transpose(1, 0, 2),
        gain_spatial,
        gain_temporal,
        qkv_spatial.transpose(0, 2, 1),
        out_spatial.reshape(3, ATT, 24, D),
        qkv_temporal.transpose(0, 2, 1).reshape(9, ATT, 24, D),
        out_temporal.reshape(3, ATT, 24, D),
        fc_in.T.reshape(8, ROUNDS - ATT, 24, D),
        fc_out.reshape(8, ROUNDS - ATT, 24, D),
    )
    return result.reshape(latent.shape)


def solution(mesh):
    placed = (
        P(None, "seq", "tp", None),
        P(),
        P(None, None, "tp"),
        P(),
        P("tp", None),
        P(None, None, "tp"),
        P(),
        P("tp", None),
        P(None, "tp"),
        P("tp", None),
    )
    return jax.shard_map(
        body, mesh=mesh, in_specs=placed, out_specs=P(None, "seq", "tp", None), check_vma=False
    )
```

```python
import math

import jax
import jax.numpy as jnp
from jax import lax
from jax.experimental import pallas as pl
from jax.experimental.pallas import tpu as pltpu
from jax.sharding import PartitionSpec as P

D = 1152
H = 16
HD = 72
HW = 144
N_TP = 8
N_SEQ = 32
MESH = pl.DeviceIdType.MESH
EPS = 1e-06
SCALE = 1.0 / math.sqrt(HD)
F32 = jnp.float32
BF16 = jnp.bfloat16

ATT = 2
ROUNDS = 5
WIDE = ()


def layer_norm(values):
    average = jnp.mean(values, axis=-1, keepdims=True)
    centred = values - average
    variance = jnp.mean(centred * centred, axis=-1, keepdims=True)
    return centred * lax.rsqrt(variance + EPS)


def dot(left, right, left_dim=1, right_dim=0):
    return lax.dot_general(
        left, right, (((left_dim,), (right_dim,)), ((), ())), preferred_element_type=F32
    )


def head_norm_rows(values, gain):
    halves = []
    for head in range(2):
        part = values[head * HD : (head + 1) * HD]
        halves.append(part * lax.rsqrt(jnp.mean(part * part, axis=0, keepdims=True) + EPS))
    return jnp.concatenate(halves, axis=0) * gain


def head_norm_lanes(values, gain):
    first = lax.broadcasted_iota(jnp.int32, values.shape, 1) < HD
    square = values * values
    low = jnp.sum(jnp.where(first, square, 0.0), axis=-1, keepdims=True)
    high = jnp.sum(jnp.where(first, 0.0, square), axis=-1, keepdims=True)
    factor = jnp.where(
        first, lax.rsqrt(low * (1.0 / HD) + EPS), lax.rsqrt(high * (1.0 / HD) + EPS)
    )
    return values * factor * gain


def remote(src, dst, send_sem, recv_sem, seq, tp):
    return pltpu.make_async_remote_copy(
        src_ref=src,
        dst_ref=dst,
        send_sem=send_sem,
        recv_sem=recv_sem,
        device_id={"seq": seq, "tp": tp},
        device_id_type=MESH,
    )


def scope(name):
    return jax.named_scope(name)


def block_kernel(
    lat,
    mod,
    gain_s,
    gain_t,
    wqkv,
    src_os,
    src_qkv,
    src_ot,
    src_1,
    src_2,
    result,
    xs,
    ks,
    qs,
    vs,
    ot,
    heads,
    ga,
    gm,
    mid,
    nrm,
    rows_in,
    rows_out,
    rows_back,
    tt,
    nm,
    total,
    part_out,
    part_in,
    ag_send,
    ag_recv,
    s1_send,
    s1_recv,
    own_sem,
    w_send,
    w_recv,
    d_send,
    d_recv,
    h_send,
    h_recv,
    x_sem,
    m_send,
    m_recv,
):
    seq, me = lax.axis_index("seq"), lax.axis_index("tp")
    x, zh, y = seq // 8, lax.rem(seq // 4, 2), lax.rem(seq, 4)
    zl, c = me // 2, lax.rem(me, 2)
    sib = zl * 2 + (1 - c)
    unit = x * 4 + y

    def xy(dx, dy):
        return (lax.rem(x + dx + 4, 4) * 2 + zh) * 4 + lax.rem(y + dy + 4, 4)

    def zdev(dz):
        z = lax.rem(zh * 4 + zl + dz + 8, 8)
        return (x * 2 + z // 4) * 4 + y, lax.rem(z, 4) * 2 + c

    ring = (xy(1, 0), xy(-1, 0), xy(0, 1), xy(0, -1))
    peers = [(seq, lax.rem(me + i, N_TP)) for i in range(1, N_TP)]
    peers += [zdev(dz) for dz in (1, -1, 2, -2)]
    barrier = pltpu.get_barrier_semaphore()

    def signal(to_seq, to_tp):
        pl.semaphore_signal(
            barrier, inc=1, device_id={"seq": to_seq, "tp": to_tp}, device_id_type=MESH
        )

    for to_seq, to_tp in peers:
        signal(to_seq, to_tp)

    def signal_seq(i, _):
        signal(lax.rem(seq + i, N_SEQ), me)
        return 0

    lax.fori_loop(1, N_SEQ, signal_seq, 0)

    def bytes_of(ref, sem):
        pltpu.make_async_copy(ref, ref, sem).wait()

    def spot(k, zs, xi, yi):
        return ga.at[zs, c, xi, yi, k] if k < ATT else gm.at[zs, xi, yi, k - ATT]

    far_z = (zl // 2) * 4 - 2

    def s1_send_to_all(k, src, dst):
        pltpu.make_async_copy(src, dst, own_sem.at[k]).start()
        for dz in (1, -1, far_z):
            remote(src, dst, s1_send.at[k], s1_recv.at[k], *zdev(dz)).start()

    def s1_start(k):
        if k in WIDE:
            return s1_start_wide(k)
        if k < ATT:
            tables = ((src_os, 0, 3), (src_qkv, 3, 12), (src_ot, 12, 16))
        else:
            tables = ((src_1, 0, 8), (src_2, 8, 16))
        for table, low, high in tables:

            @pl.when((unit >= low) & (unit < high))
            def _():
                if k < ATT:
                    src = table.at[jnp.clip(unit - low, 0, table.shape[0] - 1), k]
                else:
                    src = table.at[lax.rem(x, 2), y, k - ATT]
                s1_send_to_all(k, src, spot(k, zl, x, y))

    def s1_start_wide(k):
        j = k - ATT

        @pl.when(zl < 2)
        def _():
            s1_send_to_all(k, src_1.at[:, y, j], gm.at[zl, 0:2, y, j])
            s1_send_to_all(k, src_2.at[:, y, j], gm.at[zl, 2:4, y, j])

        for table, first in ((src_1, 0), (src_2, 2)):

            @pl.when((zl >= 2) & (x // 2 == first // 2))
            def _():
                s1_send_to_all(k, table.at[lax.rem(x, 2), :, j], gm.at[zl, x, :, j])

    def s1_bytes(k):
        return gm.at[0:3, 0, :, 0] if k in WIDE else gm.at[0, 0, 0]

    def s1_wait(k):
        bytes_of(gm.at[0, 0, :, 0] if k in WIDE else gm.at[0, 0, 0, 0], own_sem.at[k])
        bytes_of(s1_bytes(k), s1_recv.at[k])

    x_back, x_next = lax.rem(x + 3, 4), lax.rem(x + 1, 4)
    y_back, y_next = lax.rem(y + 3, 4), lax.rem(y + 1, 4)
    low, high = pl.ds(0, 2), pl.ds(2, 2)
    every = slice(None)

    def ring_copies(stage, k):
        if stage == 0:
            spots = [spot(k, low, x, y)] * 2 + [spot(k, high, x, y)] * 2
        elif stage == 1:
            spots = [
                spot(k, 0, x_back, y),
                spot(k, 1, x_next, y),
                spot(k, 2, x, y_back),
                spot(k, 3, x, y_next),
            ]
        elif stage == 2:
            spots = [spot(k, high, x, every)] * 2 + [spot(k, low, every, y)] * 2
        else:
            spots = [
                spot(k, 2, x_back, every),
                spot(k, 3, x_next, every),
                spot(k, 0, every, y_back),
                spot(k, 1, every, y_next),
            ]
        return [
            remote(there, there, w_send.at[stage, k], w_recv.at[stage, k], ring[i], me)
            for i, there in enumerate(spots)
        ]

    def ring_start(stage, k):
        for copy in ring_copies(stage, k):
            copy.start()

    def ring_wait(stage, k):
        bytes_of(ring_bytes(stage), w_recv.at[stage, k])

    def ring_bytes(stage):
        return (gm.at[:, 0, 0:2, 0], gm.at[:, 0, 0, 0], gm.at[:, 0:2, :, 0], gm.at[:, 0, :, 0])[
            stage
        ]

    def core_copy(k):
        there = ga.at[:, c, :, :, k]
        return remote(there, there, d_send.at[k], d_recv.at[k], seq, sib)

    def pump(step, k):
        with scope(f"pump_{step}_{k}"):
            if step == 0:
                s1_start(k)
            elif step == 1:
                s1_wait(k)
                ring_start(2 if k in WIDE else 0, k)
            elif step <= 4:
                ring_wait(step - 2, k)
                ring_start(step - 1, k)
            elif step == 5:
                ring_wait(3, k)
                if k < ATT:
                    core_copy(k).start()
            else:
                core_copy(k).wait_recv()

    def ag_copy(slot, b, way):
        to = (jnp.minimum(zl + 1, 3) * 2 + c, jnp.maximum(zl - 1, 0) * 2 + c, sib)[way]
        there = xs.at[slot, b]
        return remote(there, there, ag_send.at[way], ag_recv.at[slot, b], seq, to)

    def ag_step(distance, b):
        with scope(f"ag_{distance}_{b}"):
            ag_now(distance, b)

    def ag_now(distance, b):
        for way in range(2):
            origin = zl - distance if way == 0 else zl + distance
            there = (zl >= distance) if way == 0 else (zl + distance <= 3)
            more = (zl < 3) if way == 0 else (zl > 0)
            slot = origin * 2 + c

            @pl.when(there)
            def _():
                if distance > 0:
                    ag_copy(slot, b, 2).wait_recv()

                @pl.when(more)
                def _():
                    ag_copy(slot, b, way).start()

                if distance > 0 or way == 0:
                    ag_copy(slot, b, 2).start()

    def ag_drain():
        bytes_of(xs.at[0:4], ag_send.at[2])
        for z in range(4):

            @pl.when(zl == z)
            def _():
                if z < 3:
                    bytes_of(xs.at[0 : z + 1], ag_send.at[0])
                if z > 0:
                    bytes_of(xs.at[0 : 4 - z], ag_send.at[1])

    def diagonal(n):
        return lax.broadcasted_iota(jnp.int32, (n, n), 0) == lax.broadcasted_iota(
            jnp.int32, (n, n), 1
        )

    def gain_column(gains, i):
        column = jnp.where(diagonal(HD), gains[i : i + 1], 0.0)
        column = jnp.sum(column, axis=1, keepdims=True)
        return jnp.concatenate([column, column], axis=0)

    def gain_row(gains, i):
        return jnp.sum(
            jnp.where(diagonal(HW), gain_column(gains, i), 0.0), axis=0, keepdims=True
        )

    query_gain, key_gain = gain_column(gain_s, 0), gain_row(gain_s, 1)

    def project(z, b):
        with scope("project"):
            rows = xs[pl.ds(z * 2, 2), b].reshape(256, D)
            queries = head_norm_rows(dot(wqkv[0], rows, 1, 1), query_gain).astype(BF16)
            values = dot(wqkv[2], rows, 1, 1).astype(BF16)
            keys = head_norm_lanes(dot(rows, wqkv[1], 1, 1), key_gain).astype(BF16)
            for core in range(2):
                at = core * 128
                qs[b, z * 2 + core] = queries[:, at : at + 128]
                there = pl.ds(pl.multiple_of((z * 2 + core) * 128, 128), 128)
                vs[b, :, there] = values[:, at : at + 128]
                ks[b, z * 2 + core] = keys[at : at + 128]

    def take_core(z, b):
        ag_copy(z * 2 + (1 - c), b, 2).wait_recv()

    def head_copy(b, to):
        return remote(
            ot.at[b, to], heads.at[b, me], h_send.at[b], h_recv.at[b], seq, to
        )

    def attend(b, half):
        with scope(f"attend_{b}_{half}"):
            attend_now(b, half)

    def attend_now(b, half):
        keys = ks[b].reshape(N_TP * 128, HW)
        values = vs[b]

        def block(i):
            to = lax.rem(me + 1 + i, N_TP)
            query = qs[b, to].astype(F32)
            zero = jnp.zeros((HD, 128), F32)
            pair = jnp.concatenate(
                [
                    jnp.concatenate([query[:HD], zero], axis=0),
                    jnp.concatenate([zero, query[HD:]], axis=0),
                ],
                axis=1,
            ).astype(BF16)
            weights = jnp.exp(dot(keys, pair) * SCALE)
            norm = jnp.sum(weights, axis=0, keepdims=True)
            mixed = dot(values, weights.astype(BF16)) / norm
            out = jnp.concatenate([mixed[:HD, :128], mixed[HD:, 128:]], axis=0).astype(BF16)

            @pl.when(to != me)
            def _():
                ot[b, to] = out
                head_copy(b, to).start()

            @pl.when(to == me)
            def _():
                heads[b, me] = out

        def one_block(i, _):
            block(i)
            return 0

        lax.fori_loop(half * 4, half * 4 + 4, one_block, 0)

    def send_rows(source, target, send, recv, b):
        def start(i, _):
            to = lax.rem(seq + i, N_SEQ)

            @pl.when((to // 16 == b) | (b < 0))
            def _():
                remote(source.at[to], target.at[seq], send, recv, to, me).start()

            return 0

        lax.fori_loop(1, N_SEQ, start, 0)

    def take_rows(source, target, recv):
        target[seq] = source[seq]
        bytes_of(target.at[0:31], recv)

    def finish(b):
        with scope(f"finish_{b}"):
            bytes_of(heads.at[b, 0:7], h_recv.at[b])
            mixed = heads[b].reshape(D, 128).T
            out = dot(mixed, ga[:, :, 0, 0:3].reshape(D, D)).astype(BF16).astype(F32)
            rows = pl.ds(b * 128, 128)
            late = lat[rows].astype(F32) + mod[2, b : b + 1] * out
            mid[rows] = late
            normed = layer_norm(late) * (1.0 + mod[4, b : b + 1]) + mod[3, b : b + 1]
            nrm[pl.ds(b * 16, 16)] = normed.reshape(16, 8, D).astype(BF16)
            send_rows(nrm, rows_in, x_sem.at[0], x_sem.at[1], b)

    def att_rows(z, core, first):
        return jnp.concatenate(
            [ga[z, core, u // 4, u % 4].reshape(48, D) for u in range(first, first + 3)], axis=0
        )

    def temporal(half):
        rows = rows_in[...].astype(F32).reshape(256, D).astype(BF16)
        same = lax.rem(lax.broadcasted_iota(jnp.int32, (256, 256), 0), 8) == lax.rem(
            lax.broadcasted_iota(jnp.int32, (256, 256), 1), 8
        )
        column, row = gain_column(gain_t, 0), gain_row(gain_t, 1)
        zero = jnp.zeros((HD, 256), F32)

        def pair_of_heads(t):
            z, core = t // 2, lax.rem(t, 2)
            queries = head_norm_rows(dot(att_rows(z, core, 3), rows, 1, 1), column)
            keys = head_norm_lanes(dot(rows, att_rows(z, core, 6), 1, 1), row).astype(BF16)
            values = dot(att_rows(z, core, 9), rows, 1, 1).astype(BF16)
            parts = []
            for head in range(2):
                kept = queries[head * HD : (head + 1) * HD]
                kept = jnp.concatenate([kept, zero] if head == 0 else [zero, kept], axis=0)
                probs = jnp.where(same, jnp.exp(dot(keys, kept.astype(BF16)) * SCALE), 0.0)
                norm = jnp.sum(probs, axis=0, keepdims=True)
                mixed = dot(values, probs.astype(BF16)) / norm
                parts.append(mixed[head * HD : (head + 1) * HD])
            return jnp.concatenate(parts, axis=0).astype(BF16)

        def two_pairs(i, _):
            first, second = pair_of_heads(2 * i), pair_of_heads(2 * i + 1)
            tt[2 * i] = first
            tt[2 * i + 1] = second
            return 0

        lax.fori_loop(half * 2, half * 2 + 2, two_pairs, 0)
        if half == 0:
            return
        out = dot(tt[...].reshape(D, 256).T, ga[:, :, 3, 0:3].reshape(D, D))
        rows_out[...] = out.reshape(N_SEQ, 8, D).astype(BF16)

    def half_copy():
        return remote(nm.at[c], nm.at[c], m_send.at[0], m_recv.at[0], seq, sib)

    def part_copy():
        return remote(part_out, part_in, m_send.at[1], m_recv.at[1], seq, sib)

    def mlp_entry():
        back = rows_back[...].astype(F32).reshape(256, D)
        for b in range(2):
            rows = pl.ds(b * 128, 128)
            late = mid[rows] + mod[5, b : b + 1] * back[b * 128 : (b + 1) * 128]
            mid[rows] = late
            normed = layer_norm(late) * (1.0 + mod[7, b : b + 1]) + mod[6, b : b + 1]
            nm[c, rows] = normed.astype(BF16)

    def mlp_round(k, which):
        u = dot(nm[which], gm[:, 0:2, :, k].reshape(768, D), 1, 1)
        h = 0.5 * u * (1.0 + jnp.tanh(math.sqrt(2.0 / math.pi) * (u + 0.044715 * (u * u * u))))
        product = dot(h.astype(BF16), gm[:, 2:4, :, k].reshape(768, D))
        return product if k == 0 else total[which] + product

    for b in range(2):
        rows = lat[pl.ds(b * 128, 128)].astype(F32)
        xs[me, b] = (layer_norm(rows) * (1.0 + mod[1, b : b + 1]) + mod[0, b : b + 1]).astype(BF16)
    with scope("greet"):
        pl.semaphore_wait(barrier, len(peers) + N_SEQ - 1)
    near = zl + 1 - 2 * lax.rem(zl, 2)
    middle = 2 - zl // 2
    far = 3 - 3 * (zl // 2)
    pump(0, 0)
    pump(0, 1)
    ag_step(0, 0)
    ag_step(0, 1)
    for b in range(2):
        take_core(zl, b)
        project(zl, b)
    pump(1, 0)
    pump(1, 1)
    pump(2, 0)
    pump(2, 1)
    pump(3, 0)
    pump(0, 2)
    ag_step(1, 0)
    pump(3, 1)
    take_core(near, 0)
    project(near, 0)
    ag_step(1, 1)
    take_core(near, 1)
    project(near, 1)
    pump(0, 3)
    ag_step(2, 0)
    pump(4, 0)
    take_core(middle, 0)
    project(middle, 0)
    pump(1, 2)
    ag_step(2, 1)
    take_core(middle, 1)
    project(middle, 1)
    pump(4, 1)
    pump(1, 3)
    pump(2, 2)
    ag_step(3, 0)
    take_core(far, 0)
    pump(5, 0)
    project(far, 0)
    attend(0, 0)
    pump(3, 2)
    attend(0, 1)
    pump(2, 3)
    ag_step(3, 1)
    take_core(far, 1)
    pump(5, 1)
    pump(0, 4)
    project(far, 1)
    attend(1, 0)
    attend(1, 1)
    pump(4, 2)
    pump(6, 0)
    pump(6, 1)
    finish(0)
    finish(1)
    pump(1, 4)
    pump(3, 3)
    with scope("take_1"):
        take_rows(nrm, rows_in, x_sem.at[1])
    with scope("temporal"):
        temporal(0)
    pump(2, 4)
    with scope("temporal"):
        temporal(1)
    send_rows(rows_out, rows_back, x_sem.at[2], x_sem.at[3], -1)
    pump(3, 4)
    pump(4, 3)
    pump(5, 2)
    with scope("take_2"):
        take_rows(rows_out, rows_back, x_sem.at[3])
    with scope("entry"):
        mlp_entry()
        half_copy().start()
    with scope("mlp"):
        total[c] = mlp_round(0, c)
        half_copy().wait_recv()
        total[1 - c] = mlp_round(0, 1 - c)
    pump(4, 4)
    pump(5, 3)
    with scope("mlp"):
        total[c] = mlp_round(1, c)
        total[1 - c] = mlp_round(1, 1 - c)
    pump(5, 4)
    with scope("mlp"):
        part_out[...] = mlp_round(2, 1 - c).astype(BF16)
        part_copy().start()
        total[c] = mlp_round(2, c)
    with scope("last"):
        part_copy().wait_recv()
        for b in range(2):
            rows = pl.ds(b * 128, 128)
            out = (total[c, rows] + part_in[rows].astype(F32)).astype(BF16).astype(F32)
            result[rows] = (mid[rows] + mod[8, b : b + 1] * out).astype(BF16)

    with scope("drain"):
        half_copy().wait_send()
        part_copy().wait_send()
        bytes_of(nrm.at[0:31], x_sem.at[0])
        bytes_of(rows_out.at[0:31], x_sem.at[2])
        ag_drain()
        for b in range(2):
            bytes_of(ot.at[b, 0:7], h_send.at[b])
        for k in range(ROUNDS):
            bytes_of(s1_bytes(k), s1_send.at[k])
            for stage in range(2 if k in WIDE else 0, 4):
                bytes_of(ring_bytes(stage), w_send.at[stage, k])
            if k < ATT:
                core_copy(k).wait_send()


def body(
    latent,
    modulation,
    qkv_spatial,
    gain_spatial,
    out_spatial,
    qkv_temporal,
    gain_temporal,
    out_temporal,
    fc_in,
    fc_out,
):
    vmem = pl.BlockSpec(memory_space=pltpu.VMEM)
    hbm = pl.BlockSpec(memory_space=pl.ANY)
    dma = pltpu.SemaphoreType.DMA
    result = pl.pallas_call(
        block_kernel,
        name="block",
        out_shape=jax.ShapeDtypeStruct((256, D), BF16),
        in_specs=[vmem] * 5 + [hbm] * 5,
        out_specs=vmem,
        scratch_shapes=[
            pltpu.VMEM((N_TP, 2, 128, D), BF16),
            pltpu.VMEM((2, N_TP, 128, HW), BF16),
            pltpu.VMEM((2, N_TP, HW, 128), BF16),
            pltpu.VMEM((2, HW, 1024), BF16),
            pltpu.VMEM((2, N_TP, HW, 128), BF16),
            pltpu.VMEM((2, N_TP, HW, 128), BF16),
            pltpu.VMEM((4, 2, 4, 4, ATT, 24, D), BF16),
            pltpu.VMEM((4, 4, 4, ROUNDS - ATT, 24, D), BF16),
            pltpu.VMEM((256, D), F32),
            pltpu.VMEM((N_SEQ, 8, D), BF16),
            pltpu.VMEM((N_SEQ, 8, D), BF16),
            pltpu.VMEM((N_SEQ, 8, D), BF16),
            pltpu.VMEM((N_SEQ, 8, D), BF16),
            pltpu.VMEM((N_TP, HW, 256), BF16),
            pltpu.VMEM((2, 256, D), BF16),
            pltpu.VMEM((2, 256, D), F32),
            pltpu.VMEM((256, D), BF16),
            pltpu.VMEM((256, D), BF16),
            dma((3,)),
            dma((N_TP, 2)),
            dma((ROUNDS,)),
            dma((ROUNDS,)),
            dma((ROUNDS,)),
            dma((4, ROUNDS)),
            dma((4, ROUNDS)),
            dma((ATT,)),
            dma((ATT,)),
            dma((2,)),
            dma((2,)),
            dma((4,)),
            dma((2,)),
            dma((2,)),
        ],
        compiler_params=pltpu.CompilerParams(
            collective_id=0, has_side_effects=True, vmem_limit_bytes=54 << 20
        ),
    )(
        latent.reshape(256, D),
        modulation.transpose(1, 0, 2),
        gain_spatial,
        gain_temporal,
        qkv_spatial.transpose(0, 2, 1),
        out_spatial.reshape(3, ATT, 24, D),
        qkv_temporal.transpose(0, 2, 1).reshape(9, ATT, 24, D),
        out_temporal.reshape(3, ATT, 24, D),
        fc_in.T.reshape(2, 4, ROUNDS - ATT, 24, D),
        fc_out.reshape(2, 4, ROUNDS - ATT, 24, D),
    )
    return result.reshape(latent.shape)


def solution(mesh):
    placed = (
        P(None, "seq", "tp", None),
        P(),
        P(None, None, "tp"),
        P(),
        P("tp", None),
        P(None, None, "tp"),
        P(),
        P("tp", None),
        P(None, "tp"),
        P("tp", None),
    )
    return jax.shard_map(
        body, mesh=mesh, in_specs=placed, out_specs=P(None, "seq", "tp", None), check_vma=False
    )
```

```python
import math

import jax
import jax.numpy as jnp
from jax import lax
from jax.experimental import pallas as pl
from jax.experimental.pallas import tpu as pltpu
from jax.sharding import PartitionSpec as P

D = 1152
H = 16
HD = 72
HW = 144
N_TP = 8
N_SEQ = 32
MESH = pl.DeviceIdType.MESH
EPS = 1e-06
SCALE = 1.0 / math.sqrt(HD)
F32 = jnp.float32
BF16 = jnp.bfloat16

ATT = 2
MLP_ROWS = (32, 32, 8)
ROUNDS = ATT + len(MLP_ROWS)


def layer_norm(values):
    average = jnp.mean(values, axis=-1, keepdims=True)
    centred = values - average
    variance = jnp.mean(centred * centred, axis=-1, keepdims=True)
    return centred * lax.rsqrt(variance + EPS)


def dot(left, right, left_dim=1, right_dim=0):
    return lax.dot_general(
        left, right, (((left_dim,), (right_dim,)), ((), ())), preferred_element_type=F32
    )


def head_norm_rows(values, gain):
    halves = []
    for head in range(2):
        part = values[head * HD : (head + 1) * HD]
        halves.append(part * lax.rsqrt(jnp.mean(part * part, axis=0, keepdims=True) + EPS))
    return jnp.concatenate(halves, axis=0) * gain


def head_norm_lanes(values, gain):
    first = lax.broadcasted_iota(jnp.int32, values.shape, 1) < HD
    square = values * values
    low = jnp.sum(jnp.where(first, square, 0.0), axis=-1, keepdims=True)
    high = jnp.sum(jnp.where(first, 0.0, square), axis=-1, keepdims=True)
    factor = jnp.where(
        first, lax.rsqrt(low * (1.0 / HD) + EPS), lax.rsqrt(high * (1.0 / HD) + EPS)
    )
    return values * factor * gain


def remote(src, dst, send_sem, recv_sem, seq, tp):
    return pltpu.make_async_remote_copy(
        src_ref=src,
        dst_ref=dst,
        send_sem=send_sem,
        recv_sem=recv_sem,
        device_id={"seq": seq, "tp": tp},
        device_id_type=MESH,
    )


def scope(name):
    return jax.named_scope(name)


def block_kernel(
    lat_in,
    mod_in,
    gain_s,
    gain_t,
    wqkv_in,
    src_os,
    src_qkv,
    src_ot,
    src_1,
    src_2,
    result,
    lat,
    mod,
    wqkv,
    in_sem,
    xs,
    ks,
    qs,
    vs,
    ot,
    heads,
    ga,
    gm0,
    gm1,
    gm2,
    mid,
    nrm,
    rows_in,
    rows_out,
    rows_back,
    tt,
    nm,
    total,
    part_out,
    part_in,
    ag_send,
    ag_recv,
    s1_send,
    s1_recv,
    own_sem,
    w_send,
    w_recv,
    d_send,
    d_recv,
    h_send,
    h_recv,
    x_sem,
    m_send,
    m_recv,
):
    seq, me = lax.axis_index("seq"), lax.axis_index("tp")
    x, zh, y = seq // 8, lax.rem(seq // 4, 2), lax.rem(seq, 4)
    zl, c = me // 2, lax.rem(me, 2)
    sib = zl * 2 + (1 - c)
    unit = x * 4 + y

    def xy(dx, dy):
        return (lax.rem(x + dx + 4, 4) * 2 + zh) * 4 + lax.rem(y + dy + 4, 4)

    def zdev(dz):
        z = lax.rem(zh * 4 + zl + dz + 8, 8)
        return (x * 2 + z // 4) * 4 + y, lax.rem(z, 4) * 2 + c

    ring = (xy(1, 0), xy(-1, 0), xy(0, 1), xy(0, -1))
    peers = [(seq, lax.rem(me + i, N_TP)) for i in range(1, N_TP)]
    peers += [zdev(dz) for dz in (1, -1, 2, -2)]
    barrier = pltpu.get_barrier_semaphore()

    def signal(to_seq, to_tp):
        pl.semaphore_signal(
            barrier, inc=1, device_id={"seq": to_seq, "tp": to_tp}, device_id_type=MESH
        )

    for to_seq, to_tp in peers:
        signal(to_seq, to_tp)
    loads = [
        pltpu.make_async_copy(src, dst, in_sem.at[i])
        for i, (src, dst) in enumerate(((lat_in, lat), (mod_in, mod), (wqkv_in, wqkv)))
    ]
    for load in loads:
        load.start()

    def signal_seq(i, _):
        signal(lax.rem(seq + i, N_SEQ), me)
        return 0

    lax.fori_loop(1, N_SEQ, signal_seq, 0)

    def bytes_of(ref, sem):
        pltpu.make_async_copy(ref, ref, sem).wait()

    gm = (gm0, gm1, gm2)

    def spot(k, zs, xi, yi, core=c):
        return ga.at[zs, core, xi, yi, k] if k < ATT else gm[k - ATT].at[zs, xi, yi]

    far_z = (zl // 2) * 4 - 2

    def s1_start(k):
        if k < ATT:
            tables = ((src_os, 0, 3), (src_qkv, 3, 12), (src_ot, 12, 16))
        else:
            tables = ((src_1, 0, 8), (src_2, 8, 16))
        for table, first, last in tables:

            @pl.when((unit >= first) & (unit < last))
            def _():
                if k < ATT:
                    src = table.at[jnp.clip(unit - first, 0, table.shape[0] - 1), k]
                else:
                    rows = pl.ds(sum(MLP_ROWS[: k - ATT]), MLP_ROWS[k - ATT])
                    src = table.at[lax.rem(x, 2), y, rows]
                dst = spot(k, zl, x, y)
                pltpu.make_async_copy(src, dst, own_sem.at[k]).start()
                for dz in (1, -1, far_z):
                    remote(src, dst, s1_send.at[k], s1_recv.at[k], *zdev(dz)).start()

    def s1_bytes(k):
        return spot(k, slice(0, 3), 0, 0, 0)

    def s1_wait(k):
        bytes_of(spot(k, 0, 0, 0, 0), own_sem.at[k])
        bytes_of(s1_bytes(k), s1_recv.at[k])

    x_back, x_next = lax.rem(x + 3, 4), lax.rem(x + 1, 4)
    y_back, y_next = lax.rem(y + 3, 4), lax.rem(y + 1, 4)
    low, high = pl.ds(0, 2), pl.ds(2, 2)
    every = slice(None)

    def ring_copies(stage, k):
        if stage == 0:
            spots = [spot(k, low, x, y)] * 2 + [spot(k, high, x, y)] * 2
        elif stage == 1:
            spots = [
                spot(k, 0, x_back, y),
                spot(k, 1, x_next, y),
                spot(k, 2, x, y_back),
                spot(k, 3, x, y_next),
            ]
        elif stage == 2:
            spots = [spot(k, high, x, every)] * 2 + [spot(k, low, every, y)] * 2
        else:
            spots = [
                spot(k, 2, x_back, every),
                spot(k, 3, x_next, every),
                spot(k, 0, every, y_back),
                spot(k, 1, every, y_next),
            ]
        return [
            remote(there, there, w_send.at[stage, k], w_recv.at[stage, k], ring[i], me)
            for i, there in enumerate(spots)
        ]

    def ring_start(stage, k):
        for copy in ring_copies(stage, k):
            copy.start()

    def ring_wait(stage, k):
        bytes_of(ring_bytes(stage, k), w_recv.at[stage, k])

    def ring_bytes(stage, k):
        pair = slice(0, 2)
        if stage == 0:
            return spot(k, every, 0, pair, 0)
        if stage == 1:
            return spot(k, every, 0, 0, 0)
        return spot(k, every, pair if stage == 2 else 0, every, 0)

    def core_copy(k, part):
        there = (
            ga.at[:, c, 0, 0:3, k],
            ga.at[:, c, 0, 3, k],
            ga.at[:, c, 1:4, :, k],
        )[part]
        return remote(there, there, d_send.at[k, part], d_recv.at[k, part], seq, sib)

    def pump(step, k):
        with scope(f"pump_{step}_{k}"):
            if step == 0:
                s1_start(k)
            elif step == 1:
                s1_wait(k)
                ring_start(0, k)
            elif step <= 4:
                ring_wait(step - 2, k)
                ring_start(step - 1, k)
            elif step == 5:
                ring_wait(3, k)
                if k < ATT:
                    core_copy(k, 0).start()
            elif step == 6:
                core_copy(k, 1).start()
                core_copy(k, 2).start()
            elif step == 7:
                core_copy(k, 0).wait_recv()
            else:
                core_copy(k, 1).wait_recv()
                core_copy(k, 2).wait_recv()

    def ag_copy(slot, b, way):
        to = (jnp.minimum(zl + 1, 3) * 2 + c, jnp.maximum(zl - 1, 0) * 2 + c, sib)[way]
        there = xs.at[slot, b]
        return remote(there, there, ag_send.at[way], ag_recv.at[slot, b], seq, to)

    def ag_step(distance, b):
        with scope(f"ag_{distance}_{b}"):
            ag_now(distance, b)

    def ag_now(distance, b):
        for way in range(2):
            origin = zl - distance if way == 0 else zl + distance
            there = (zl >= distance) if way == 0 else (zl + distance <= 3)
            more = (zl < 3) if way == 0 else (zl > 0)
            slot = origin * 2 + c

            @pl.when(there)
            def _():
                if distance > 0:
                    ag_copy(slot, b, 2).wait_recv()

                @pl.when(more)
                def _():
                    ag_copy(slot, b, way).start()

                if distance > 0 or way == 0:
                    ag_copy(slot, b, 2).start()

    def ag_drain():
        bytes_of(xs.at[0:4], ag_send.at[2])
        for z in range(4):

            @pl.when(zl == z)
            def _():
                if z < 3:
                    bytes_of(xs.at[0 : z + 1], ag_send.at[0])
                if z > 0:
                    bytes_of(xs.at[0 : 4 - z], ag_send.at[1])

    def diagonal(n):
        return lax.broadcasted_iota(jnp.int32, (n, n), 0) == lax.broadcasted_iota(
            jnp.int32, (n, n), 1
        )

    def gain_column(gains, i):
        column = jnp.where(diagonal(HD), gains[i : i + 1], 0.0)
        column = jnp.sum(column, axis=1, keepdims=True)
        return jnp.concatenate([column, column], axis=0)

    def gain_row(gains, i):
        return jnp.sum(
            jnp.where(diagonal(HW), gain_column(gains, i), 0.0), axis=0, keepdims=True
        )

    query_gain, key_gain = gain_column(gain_s, 0), gain_row(gain_s, 1)

    def project(z, b):
        with scope("project"):
            rows = xs[pl.ds(z * 2, 2), b].reshape(256, D)
            queries = head_norm_rows(dot(wqkv[0], rows, 1, 1), query_gain).astype(BF16)
            values = dot(wqkv[2], rows, 1, 1).astype(BF16)
            keys = head_norm_lanes(dot(rows, wqkv[1], 1, 1), key_gain).astype(BF16)
            for core in range(2):
                at = core * 128
                qs[b, z * 2 + core] = queries[:, at : at + 128]
                there = pl.ds(pl.multiple_of((z * 2 + core) * 128, 128), 128)
                vs[b, :, there] = values[:, at : at + 128]
                ks[b, z * 2 + core] = keys[at : at + 128]

    def take_core(z, b):
        ag_copy(z * 2 + (1 - c), b, 2).wait_recv()

    def head_copy(b, to):
        return remote(
            ot.at[b, to], heads.at[b, me], h_send.at[b], h_recv.at[b], seq, to
        )

    def attend(b, half):
        with scope(f"attend_{b}_{half}"):
            attend_now(b, half)

    def attend_now(b, half):
        keys = ks[b].reshape(N_TP * 128, HW)
        values = vs[b]

        def block(i):
            to = lax.rem(me + 1 + i, N_TP)
            query = qs[b, to].astype(F32)
            zero = jnp.zeros((HD, 128), F32)
            pair = jnp.concatenate(
                [
                    jnp.concatenate([query[:HD], zero], axis=0),
                    jnp.concatenate([zero, query[HD:]], axis=0),
                ],
                axis=1,
            ).astype(BF16)
            weights = jnp.exp(dot(keys, pair) * SCALE)
            norm = jnp.sum(weights, axis=0, keepdims=True)
            mixed = dot(values, weights.astype(BF16)) / norm
            out = jnp.concatenate([mixed[:HD, :128], mixed[HD:, 128:]], axis=0).astype(BF16)

            @pl.when(to != me)
            def _():
                ot[b, to] = out
                head_copy(b, to).start()

            @pl.when(to == me)
            def _():
                heads[b, me] = out

        def one_block(i, _):
            block(i)
            return 0

        lax.fori_loop(half * 4, half * 4 + 4, one_block, 0)

    def send_rows(source, target, send, recv, b):
        for other in (1, 0):

            def start(i, _):
                to_x, to_y = lax.rem(x + i // 4, 4), lax.rem(y + i, 4)
                to = (to_x * 2 + lax.rem(zh + other, 2)) * 4 + to_y

                @pl.when((to // 16 == b) | (b < 0))
                def _():
                    remote(source.at[to], target.at[seq], send, recv, to, me).start()

                return 0

            lax.fori_loop(1 - other, 16, start, 0)

    def take_rows(source, target, recv):
        target[seq] = source[seq]
        bytes_of(target.at[0:31], recv)

    def finish(b):
        with scope(f"finish_{b}"):
            mixed = heads[b].reshape(D, 128).T
            out = dot(mixed, ga[:, :, 0, 0:3].reshape(D, D)).astype(BF16).astype(F32)
            rows = pl.ds(b * 128, 128)
            late = lat[rows].astype(F32) + mod[2, b : b + 1] * out
            mid[rows] = late
            normed = layer_norm(late) * (1.0 + mod[4, b : b + 1]) + mod[3, b : b + 1]
            nrm[pl.ds(b * 16, 16)] = normed.reshape(16, 8, D).astype(BF16)
            send_rows(nrm, rows_in, x_sem.at[0], x_sem.at[1], b)

    def att_rows(z, core, first):
        return jnp.concatenate(
            [ga[z, core, u // 4, u % 4].reshape(48, D) for u in range(first, first + 3)], axis=0
        )

    def temporal():
        rows = rows_in[...].astype(F32).reshape(256, D).astype(BF16)
        same = lax.rem(lax.broadcasted_iota(jnp.int32, (256, 256), 0), 8) == lax.rem(
            lax.broadcasted_iota(jnp.int32, (256, 256), 1), 8
        )
        column, row = gain_column(gain_t, 0), gain_row(gain_t, 1)
        zero = jnp.zeros((HD, 256), F32)

        def pair_of_heads(t):
            z, core = t // 2, lax.rem(t, 2)
            table = jnp.concatenate([att_rows(z, core, 3), att_rows(z, core, 9)], axis=0)
            both = dot(table, rows, 1, 1)
            queries = head_norm_rows(both[:HW], column)
            keys = head_norm_lanes(dot(rows, att_rows(z, core, 6), 1, 1), row).astype(BF16)
            values = both[HW:].astype(BF16)
            parts = []
            for head in range(2):
                kept = queries[head * HD : (head + 1) * HD]
                kept = jnp.concatenate([kept, zero] if head == 0 else [zero, kept], axis=0)
                probs = jnp.where(same, jnp.exp(dot(keys, kept.astype(BF16)) * SCALE), 0.0)
                norm = jnp.sum(probs, axis=0, keepdims=True)
                mixed = dot(values, probs.astype(BF16)) / norm
                parts.append(mixed[head * HD : (head + 1) * HD])
            return jnp.concatenate(parts, axis=0).astype(BF16)

        def four_pairs(i, _):
            done = [pair_of_heads(4 * i + j) for j in range(4)]
            for j in range(4):
                tt[4 * i + j] = done[j]
            return 0

        lax.fori_loop(0, 2, four_pairs, 0)
        out = dot(tt[...].reshape(D, 256).T, ga[:, :, 3, 0:3].reshape(D, D))
        rows_out[...] = out.reshape(N_SEQ, 8, D).astype(BF16)

    def half_copy():
        return remote(nm.at[c], nm.at[c], m_send.at[0], m_recv.at[0], seq, sib)

    def part_copy():
        return remote(part_out, part_in, m_send.at[1], m_recv.at[1], seq, sib)

    def mlp_entry():
        back = rows_back[...].astype(F32).reshape(256, D)
        for b in range(2):
            rows = pl.ds(b * 128, 128)
            late = mid[rows] + mod[5, b : b + 1] * back[b * 128 : (b + 1) * 128]
            mid[rows] = late
            normed = layer_norm(late) * (1.0 + mod[7, b : b + 1]) + mod[6, b : b + 1]
            nm[c, rows] = normed.astype(BF16)

    def mlp_round(k, which):
        u = dot(nm[which], gm[k][:, 0:2].reshape(32 * MLP_ROWS[k], D), 1, 1)
        h = 0.5 * u * (1.0 + jnp.tanh(math.sqrt(2.0 / math.pi) * (u + 0.044715 * (u * u * u))))
        product = dot(h.astype(BF16), gm[k][:, 2:4].reshape(32 * MLP_ROWS[k], D))
        return product if k == 0 else total[which] + product

    near = zl + 1 - 2 * lax.rem(zl, 2)
    middle = 2 - zl // 2
    far = 3 - 3 * (zl // 2)
    with scope("greet"):
        pl.semaphore_wait(barrier, len(peers) + N_SEQ - 1)
    pump(0, 0)
    pump(0, 1)
    loads[0].wait()
    loads[1].wait()
    for b in range(2):
        rows = lat[pl.ds(b * 128, 128)].astype(F32)
        xs[me, b] = (layer_norm(rows) * (1.0 + mod[1, b : b + 1]) + mod[0, b : b + 1]).astype(BF16)
        ag_step(0, b)
    pump(1, 0)
    loads[2].wait()
    take_core(zl, 0)
    project(zl, 0)
    pump(1, 1)
    take_core(zl, 1)
    project(zl, 1)
    pump(2, 0)
    pump(2, 1)
    pump(3, 0)
    ag_step(1, 0)
    pump(3, 1)
    take_core(near, 0)
    project(near, 0)
    ag_step(1, 1)
    take_core(near, 1)
    project(near, 1)
    ag_step(2, 0)
    pump(0, 2)
    pump(4, 0)
    take_core(middle, 0)
    project(middle, 0)
    ag_step(2, 1)
    pump(0, 3)
    pump(0, 4)
    take_core(middle, 1)
    project(middle, 1)
    pump(4, 1)
    pump(1, 2)
    ag_step(3, 0)
    take_core(far, 0)
    pump(5, 0)
    project(far, 0)
    attend(0, 0)
    pump(2, 2)
    attend(0, 1)
    ag_step(3, 1)
    pump(3, 2)
    take_core(far, 1)
    pump(5, 1)
    pump(6, 0)
    pump(6, 1)
    project(far, 1)
    attend(1, 0)
    attend(1, 1)
    pump(1, 3)
    pump(1, 4)
    pump(7, 0)
    pump(7, 1)
    with scope("take_heads"):
        for b in range(2):
            bytes_of(heads.at[b, 0:7], h_recv.at[b])
    finish(0)
    finish(1)
    pump(4, 2)
    pump(2, 3)
    pump(2, 4)
    pump(3, 3)
    with scope("take_1"):
        take_rows(nrm, rows_in, x_sem.at[1])
    pump(8, 0)
    pump(8, 1)
    with scope("temporal"):
        temporal()
    send_rows(rows_out, rows_back, x_sem.at[2], x_sem.at[3], -1)
    pump(3, 4)
    pump(4, 3)
    pump(4, 4)
    with scope("take_2"):
        take_rows(rows_out, rows_back, x_sem.at[3])
    with scope("entry"):
        mlp_entry()
        half_copy().start()
    pump(5, 2)
    with scope("mlp"):
        total[c] = mlp_round(0, c)
        half_copy().wait_recv()
        total[1 - c] = mlp_round(0, 1 - c)
    pump(5, 3)
    with scope("mlp"):
        total[c] = mlp_round(1, c)
        total[1 - c] = mlp_round(1, 1 - c)
    pump(5, 4)
    with scope("mlp"):
        part_out[...] = mlp_round(2, 1 - c).astype(BF16)
        part_copy().start()
        total[c] = mlp_round(2, c)
    with scope("last"):
        part_copy().wait_recv()
        for b in range(2):
            rows = pl.ds(b * 128, 128)
            out = (total[c, rows] + part_in[rows].astype(F32)).astype(BF16).astype(F32)
            result[rows] = (mid[rows] + mod[8, b : b + 1] * out).astype(BF16)

    with scope("drain"):
        half_copy().wait_send()
        part_copy().wait_send()
        bytes_of(nrm.at[0:31], x_sem.at[0])
        bytes_of(rows_out.at[0:31], x_sem.at[2])
        ag_drain()
        for b in range(2):
            bytes_of(ot.at[b, 0:7], h_send.at[b])
        for k in range(ROUNDS):
            bytes_of(s1_bytes(k), s1_send.at[k])
            for stage in range(4):
                bytes_of(ring_bytes(stage, k), w_send.at[stage, k])
            if k < ATT:
                for part in range(3):
                    core_copy(k, part).wait_send()


def body(
    latent,
    modulation,
    qkv_spatial,
    gain_spatial,
    out_spatial,
    qkv_temporal,
    gain_temporal,
    out_temporal,
    fc_in,
    fc_out,
):
    vmem = pl.BlockSpec(memory_space=pltpu.VMEM)
    hbm = pl.BlockSpec(memory_space=pl.ANY)
    dma = pltpu.SemaphoreType.DMA
    result = pl.pallas_call(
        block_kernel,
        name="block",
        out_shape=jax.ShapeDtypeStruct((256, D), BF16),
        in_specs=[hbm] * 2 + [vmem] * 2 + [hbm] * 6,
        out_specs=vmem,
        scratch_shapes=[
            pltpu.VMEM((256, D), BF16),
            pltpu.VMEM((9, 2, D), F32),
            pltpu.VMEM((3, HW, D), BF16),
            dma((3,)),
            pltpu.VMEM((N_TP, 2, 128, D), BF16),
            pltpu.VMEM((2, N_TP, 128, HW), BF16),
            pltpu.VMEM((2, N_TP, HW, 128), BF16),
            pltpu.VMEM((2, HW, 1024), BF16),
            pltpu.VMEM((2, N_TP, HW, 128), BF16),
            pltpu.VMEM((2, N_TP, HW, 128), BF16),
            pltpu.VMEM((4, 2, 4, 4, ATT, 24, D), BF16),
            *[pltpu.VMEM((4, 4, 4, rows, D), BF16) for rows in MLP_ROWS],
            pltpu.VMEM((256, D), F32),
            pltpu.VMEM((N_SEQ, 8, D), BF16),
            pltpu.VMEM((N_SEQ, 8, D), BF16),
            pltpu.VMEM((N_SEQ, 8, D), BF16),
            pltpu.VMEM((N_SEQ, 8, D), BF16),
            pltpu.VMEM((N_TP, HW, 256), BF16),
            pltpu.VMEM((2, 256, D), BF16),
            pltpu.VMEM((2, 256, D), F32),
            pltpu.VMEM((256, D), BF16),
            pltpu.VMEM((256, D), BF16),
            dma((3,)),
            dma((N_TP, 2)),
            dma((ROUNDS,)),
            dma((ROUNDS,)),
            dma((ROUNDS,)),
            dma((4, ROUNDS)),
            dma((4, ROUNDS)),
            dma((ATT, 3)),
            dma((ATT, 3)),
            dma((2,)),
            dma((2,)),
            dma((4,)),
            dma((2,)),
            dma((2,)),
        ],
        compiler_params=pltpu.CompilerParams(
            collective_id=0, has_side_effects=True, vmem_limit_bytes=54 << 20
        ),
    )(
        latent.reshape(256, D),
        modulation.transpose(1, 0, 2),
        gain_spatial,
        gain_temporal,
        qkv_spatial.transpose(0, 2, 1),
        out_spatial.reshape(3, ATT, 24, D),
        qkv_temporal.transpose(0, 2, 1).reshape(9, ATT, 24, D),
        out_temporal.reshape(3, ATT, 24, D),
        fc_in.T.reshape(2, 4, 72, D),
        fc_out.reshape(2, 4, 72, D),
    )
    return result.reshape(latent.shape)


def solution(mesh):
    placed = (
        P(None, "seq", "tp", None),
        P(),
        P(None, None, "tp"),
        P(),
        P("tp", None),
        P(None, None, "tp"),
        P(),
        P("tp", None),
        P(None, "tp"),
        P("tp", None),
    )
    return jax.shard_map(
        body, mesh=mesh, in_specs=placed, out_specs=P(None, "seq", "tp", None), check_vma=False
    )
```

```python
import math

import jax
import jax.numpy as jnp
from jax import lax
from jax.experimental import pallas as pl
from jax.experimental.pallas import tpu as pltpu
from jax.sharding import PartitionSpec as P

D = 1152
H = 16
HD = 72
HW = 144
N_TP = 8
N_SEQ = 32
MESH = pl.DeviceIdType.MESH
EPS = 1e-06
SCALE = 1.0 / math.sqrt(HD)
F32 = jnp.float32
BF16 = jnp.bfloat16

ATT = 2
MLP_ROWS = (32, 32, 8)
ROUNDS = ATT + len(MLP_ROWS)


def layer_norm(values):
    average = jnp.mean(values, axis=-1, keepdims=True)
    centred = values - average
    variance = jnp.mean(centred * centred, axis=-1, keepdims=True)
    return centred * lax.rsqrt(variance + EPS)


def dot(left, right, left_dim=1, right_dim=0):
    return lax.dot_general(
        left, right, (((left_dim,), (right_dim,)), ((), ())), preferred_element_type=F32
    )


def head_norm_rows(values, gain):
    halves = []
    for head in range(2):
        part = values[head * HD : (head + 1) * HD]
        halves.append(part * lax.rsqrt(jnp.mean(part * part, axis=0, keepdims=True) + EPS))
    return jnp.concatenate(halves, axis=0) * gain


def head_norm_lanes(values, gain):
    first = lax.broadcasted_iota(jnp.int32, values.shape, 1) < HD
    square = values * values
    low = jnp.sum(jnp.where(first, square, 0.0), axis=-1, keepdims=True)
    high = jnp.sum(jnp.where(first, 0.0, square), axis=-1, keepdims=True)
    factor = jnp.where(
        first, lax.rsqrt(low * (1.0 / HD) + EPS), lax.rsqrt(high * (1.0 / HD) + EPS)
    )
    return values * factor * gain


def remote(src, dst, send_sem, recv_sem, seq, tp):
    return pltpu.make_async_remote_copy(
        src_ref=src,
        dst_ref=dst,
        send_sem=send_sem,
        recv_sem=recv_sem,
        device_id={"seq": seq, "tp": tp},
        device_id_type=MESH,
    )


def scope(name):
    return jax.named_scope(name)


def block_kernel(
    lat_in,
    mod_in,
    gain_s,
    gain_t,
    wqkv_in,
    src_os,
    src_qkv,
    src_ot,
    src_1,
    src_2,
    result,
    lat,
    mod,
    wqkv,
    in_sem,
    xs,
    ks,
    qs,
    vs,
    ot,
    heads,
    ga,
    gm0,
    gm1,
    gm2,
    mid,
    nrm,
    rows_in,
    rows_out,
    rows_back,
    tt,
    nm,
    total,
    part_out,
    part_in,
    ag_send,
    ag_recv,
    s1_send,
    s1_recv,
    own_sem,
    w_send,
    w_recv,
    d_send,
    d_recv,
    h_send,
    h_recv,
    x_sem,
    m_send,
    m_recv,
):
    seq, me = lax.axis_index("seq"), lax.axis_index("tp")
    x, zh, y = seq // 8, lax.rem(seq // 4, 2), lax.rem(seq, 4)
    zl, c = me // 2, lax.rem(me, 2)
    sib = zl * 2 + (1 - c)
    unit = x * 4 + y

    def xy(dx, dy):
        return (lax.rem(x + dx + 4, 4) * 2 + zh) * 4 + lax.rem(y + dy + 4, 4)

    def zdev(dz):
        z = lax.rem(zh * 4 + zl + dz + 8, 8)
        return (x * 2 + z // 4) * 4 + y, lax.rem(z, 4) * 2 + c

    ring = (xy(1, 0), xy(-1, 0), xy(0, 1), xy(0, -1))
    peers = [(seq, lax.rem(me + i, N_TP)) for i in range(1, N_TP)]
    peers += [zdev(dz) for dz in (1, -1, 2, -2)]
    barrier = pltpu.get_barrier_semaphore()

    def signal(to_seq, to_tp):
        pl.semaphore_signal(
            barrier, inc=1, device_id={"seq": to_seq, "tp": to_tp}, device_id_type=MESH
        )

    for to_seq, to_tp in peers:
        signal(to_seq, to_tp)
    loads = [
        pltpu.make_async_copy(src, dst, in_sem.at[i])
        for i, (src, dst) in enumerate(((lat_in, lat), (mod_in, mod), (wqkv_in, wqkv)))
    ]
    for load in loads:
        load.start()

    def signal_seq(i, _):
        signal(lax.rem(seq + i, N_SEQ), me)
        return 0

    lax.fori_loop(1, N_SEQ, signal_seq, 0)

    def bytes_of(ref, sem):
        pltpu.make_async_copy(ref, ref, sem).wait()

    gm = (gm0, gm1, gm2)

    def spot(k, zs, xi, yi, core=c):
        return ga.at[zs, core, xi, yi, k] if k < ATT else gm[k - ATT].at[zs, xi, yi]

    far_z = (zl // 2) * 4 - 2

    def s1_start(k):
        if k < ATT:
            tables = ((src_os, 0, 3), (src_qkv, 3, 12), (src_ot, 12, 16))
        else:
            tables = ((src_1, 0, 8), (src_2, 8, 16))
        for table, first, last in tables:

            @pl.when((unit >= first) & (unit < last))
            def _():
                if k < ATT:
                    src = table.at[jnp.clip(unit - first, 0, table.shape[0] - 1), k]
                else:
                    rows = pl.ds(sum(MLP_ROWS[: k - ATT]), MLP_ROWS[k - ATT])
                    src = table.at[lax.rem(x, 2), y, rows]
                dst = spot(k, zl, x, y)
                pltpu.make_async_copy(src, dst, own_sem.at[k]).start()
                for dz in (1, -1, far_z):
                    remote(src, dst, s1_send.at[k], s1_recv.at[k], *zdev(dz)).start()

    def s1_bytes(k):
        return spot(k, slice(0, 3), 0, 0, 0)

    def s1_wait(k):
        bytes_of(spot(k, 0, 0, 0, 0), own_sem.at[k])
        bytes_of(s1_bytes(k), s1_recv.at[k])

    x_back, x_next = lax.rem(x + 3, 4), lax.rem(x + 1, 4)
    y_back, y_next = lax.rem(y + 3, 4), lax.rem(y + 1, 4)
    low, high = pl.ds(0, 2), pl.ds(2, 2)
    every = slice(None)

    def ring_copies(stage, k):
        if stage == 0:
            spots = [spot(k, low, x, y)] * 2 + [spot(k, high, x, y)] * 2
        elif stage == 1:
            spots = [
                spot(k, 0, x_back, y),
                spot(k, 1, x_next, y),
                spot(k, 2, x, y_back),
                spot(k, 3, x, y_next),
            ]
        elif stage == 2:
            spots = [spot(k, high, x, every)] * 2 + [spot(k, low, every, y)] * 2
        else:
            spots = [
                spot(k, 2, x_back, every),
                spot(k, 3, x_next, every),
                spot(k, 0, every, y_back),
                spot(k, 1, every, y_next),
            ]
        return [
            remote(there, there, w_send.at[stage, k], w_recv.at[stage, k], ring[i], me)
            for i, there in enumerate(spots)
        ]

    def ring_start(stage, k):
        for copy in ring_copies(stage, k):
            copy.start()

    def ring_wait(stage, k):
        bytes_of(ring_bytes(stage, k), w_recv.at[stage, k])

    def ring_bytes(stage, k):
        pair = slice(0, 2)
        if stage == 0:
            return spot(k, every, 0, pair, 0)
        if stage == 1:
            return spot(k, every, 0, 0, 0)
        return spot(k, every, pair if stage == 2 else 0, every, 0)

    def core_copy(k, part):
        there = (
            ga.at[:, c, 0, 0:3, k],
            ga.at[:, c, 0, 3, k],
            ga.at[:, c, 1:4, :, k],
        )[part]
        return remote(there, there, d_send.at[k, part], d_recv.at[k, part], seq, sib)

    def pump(step, k):
        with scope(f"pump_{step}_{k}"):
            if step == 0:
                s1_start(k)
            elif step == 1:
                s1_wait(k)
                ring_start(0, k)
            elif step <= 4:
                ring_wait(step - 2, k)
                ring_start(step - 1, k)
            elif step == 5:
                ring_wait(3, k)
                if k < ATT:
                    core_copy(k, 0).start()
            elif step == 6:
                core_copy(k, 1).start()
                core_copy(k, 2).start()
            elif step == 7:
                core_copy(k, 0).wait_recv()
            else:
                core_copy(k, 1).wait_recv()
                core_copy(k, 2).wait_recv()

    def ag_copy(slot, b, way):
        to = (jnp.minimum(zl + 1, 3) * 2 + c, jnp.maximum(zl - 1, 0) * 2 + c, sib)[way]
        there = xs.at[slot, b]
        return remote(there, there, ag_send.at[way], ag_recv.at[slot, b], seq, to)

    def ag_step(distance, b):
        with scope(f"ag_{distance}_{b}"):
            ag_now(distance, b)

    def ag_now(distance, b):
        for way in range(2):
            origin = zl - distance if way == 0 else zl + distance
            there = (zl >= distance) if way == 0 else (zl + distance <= 3)
            more = (zl < 3) if way == 0 else (zl > 0)
            slot = origin * 2 + c

            @pl.when(there)
            def _():
                if distance > 0:
                    ag_copy(slot, b, 2).wait_recv()

                @pl.when(more)
                def _():
                    ag_copy(slot, b, way).start()

                if distance > 0 or way == 0:
                    ag_copy(slot, b, 2).start()

    def ag_drain():
        bytes_of(xs.at[0:4], ag_send.at[2])
        for z in range(4):

            @pl.when(zl == z)
            def _():
                if z < 3:
                    bytes_of(xs.at[0 : z + 1], ag_send.at[0])
                if z > 0:
                    bytes_of(xs.at[0 : 4 - z], ag_send.at[1])

    def diagonal(n):
        return lax.broadcasted_iota(jnp.int32, (n, n), 0) == lax.broadcasted_iota(
            jnp.int32, (n, n), 1
        )

    def gain_column(gains, i):
        column = jnp.where(diagonal(HD), gains[i : i + 1], 0.0)
        column = jnp.sum(column, axis=1, keepdims=True)
        return jnp.concatenate([column, column], axis=0)

    def gain_row(gains, i):
        return jnp.sum(
            jnp.where(diagonal(HW), gain_column(gains, i), 0.0), axis=0, keepdims=True
        )

    query_gain, key_gain = gain_column(gain_s, 0), gain_row(gain_s, 1)

    def project(z, b):
        with scope("project"):
            rows = xs[pl.ds(z * 2, 2), b].reshape(256, D)
            queries = head_norm_rows(dot(wqkv[0], rows, 1, 1), query_gain).astype(BF16)
            values = dot(wqkv[2], rows, 1, 1).astype(BF16)
            keys = head_norm_lanes(dot(rows, wqkv[1], 1, 1), key_gain).astype(BF16)
            for core in range(2):
                at = core * 128
                qs[b, z * 2 + core] = queries[:, at : at + 128]
                there = pl.ds(pl.multiple_of((z * 2 + core) * 128, 128), 128)
                vs[b, :, there] = values[:, at : at + 128]
                ks[b, z * 2 + core] = keys[at : at + 128]

    def take_core(z, b):
        ag_copy(z * 2 + (1 - c), b, 2).wait_recv()

    def head_copy(b, to):
        return remote(
            ot.at[b, to], heads.at[b, me], h_send.at[b], h_recv.at[b], seq, to
        )

    def attend(b, half):
        with scope(f"attend_{b}_{half}"):
            attend_now(b, half)

    def attend_now(b, half):
        keys = ks[b].reshape(N_TP * 128, HW)
        values = vs[b]

        def block(i):
            to = lax.rem(me + 1 + i, N_TP)
            query = qs[b, to].astype(F32)
            zero = jnp.zeros((HD, 128), F32)
            pair = jnp.concatenate(
                [
                    jnp.concatenate([query[:HD], zero], axis=0),
                    jnp.concatenate([zero, query[HD:]], axis=0),
                ],
                axis=1,
            ).astype(BF16)
            weights = jnp.exp(dot(keys, pair) * SCALE)
            norm = jnp.sum(weights, axis=0, keepdims=True)
            mixed = dot(values, weights.astype(BF16)) / norm
            out = jnp.concatenate([mixed[:HD, :128], mixed[HD:, 128:]], axis=0).astype(BF16)

            @pl.when(to != me)
            def _():
                ot[b, to] = out
                head_copy(b, to).start()

            @pl.when(to == me)
            def _():
                heads[b, me] = out

        def one_block(i, _):
            block(i)
            return 0

        lax.fori_loop(half * 4, half * 4 + 4, one_block, 0)

    def send_rows(source, target, send, recv, b):
        for other in (1, 0):

            def start(i, _):
                to_x, to_y = lax.rem(x + i // 4, 4), lax.rem(y + i, 4)
                to = (to_x * 2 + lax.rem(zh + other, 2)) * 4 + to_y

                @pl.when((to // 16 == b) | (b < 0))
                def _():
                    remote(source.at[to], target.at[seq], send, recv, to, me).start()

                return 0

            lax.fori_loop(1 - other, 16, start, 0)

    def take_rows(source, target, recv):
        target[seq] = source[seq]
        bytes_of(target.at[0:31], recv)

    def finish(b):
        with scope(f"finish_{b}"):
            mixed = heads[b].reshape(D, 128).T
            out = dot(mixed, ga[:, :, 0, 0:3].reshape(D, D)).astype(BF16).astype(F32)
            rows = pl.ds(b * 128, 128)
            late = lat[rows].astype(F32) + mod[2, b : b + 1] * out
            mid[rows] = late
            normed = layer_norm(late) * (1.0 + mod[4, b : b + 1]) + mod[3, b : b + 1]
            nrm[pl.ds(b * 16, 16)] = normed.reshape(16, 8, D).astype(BF16)
            send_rows(nrm, rows_in, x_sem.at[0], x_sem.at[1], b)

    def att_rows(z, core, first):
        return jnp.concatenate(
            [ga[z, core, u // 4, u % 4].reshape(48, D) for u in range(first, first + 3)], axis=0
        )

    def temporal():
        rows = rows_in[...].astype(F32).reshape(256, D).astype(BF16)
        same = lax.rem(lax.broadcasted_iota(jnp.int32, (256, 256), 0), 8) == lax.rem(
            lax.broadcasted_iota(jnp.int32, (256, 256), 1), 8
        )
        column, row = gain_column(gain_t, 0), gain_row(gain_t, 1)
        zero = jnp.zeros((HD, 256), F32)

        def pair_of_heads(t):
            z, core = t // 2, lax.rem(t, 2)
            table = jnp.concatenate([att_rows(z, core, 3), att_rows(z, core, 9)], axis=0)
            both = dot(table, rows, 1, 1)
            queries = head_norm_rows(both[:HW], column)
            keys = head_norm_lanes(dot(rows, att_rows(z, core, 6), 1, 1), row).astype(BF16)
            values = both[HW:].astype(BF16)
            parts = []
            for head in range(2):
                kept = queries[head * HD : (head + 1) * HD]
                kept = jnp.concatenate([kept, zero] if head == 0 else [zero, kept], axis=0)
                probs = jnp.where(same, jnp.exp(dot(keys, kept.astype(BF16)) * SCALE), 0.0)
                norm = jnp.sum(probs, axis=0, keepdims=True)
                mixed = dot(values, probs.astype(BF16)) / norm
                parts.append(mixed[head * HD : (head + 1) * HD])
            return jnp.concatenate(parts, axis=0).astype(BF16)

        def four_pairs(i, _):
            done = [pair_of_heads(4 * i + j) for j in range(4)]
            for j in range(4):
                tt[4 * i + j] = done[j]
            return 0

        lax.fori_loop(0, 2, four_pairs, 0)
        out = dot(tt[...].reshape(D, 256).T, ga[:, :, 3, 0:3].reshape(D, D))
        rows_out[...] = out.reshape(N_SEQ, 8, D).astype(BF16)

    def half_copy():
        return remote(nm.at[c], nm.at[c], m_send.at[0], m_recv.at[0], seq, sib)

    def part_copy():
        return remote(part_out, part_in, m_send.at[1], m_recv.at[1], seq, sib)

    def mlp_entry():
        back = rows_back[...].astype(F32).reshape(256, D)
        for b in range(2):
            rows = pl.ds(b * 128, 128)
            late = mid[rows] + mod[5, b : b + 1] * back[b * 128 : (b + 1) * 128]
            mid[rows] = late
            normed = layer_norm(late) * (1.0 + mod[7, b : b + 1]) + mod[6, b : b + 1]
            nm[c, rows] = normed.astype(BF16)

    def mlp_round(k, which):
        u = dot(nm[which], gm[k][:, 0:2].reshape(32 * MLP_ROWS[k], D), 1, 1)
        h = 0.5 * u * (1.0 + jnp.tanh(math.sqrt(2.0 / math.pi) * (u + 0.044715 * (u * u * u))))
        product = dot(h.astype(BF16), gm[k][:, 2:4].reshape(32 * MLP_ROWS[k], D))
        return product if k == 0 else total[which] + product

    near = zl + 1 - 2 * lax.rem(zl, 2)
    middle = 2 - zl // 2
    far = 3 - 3 * (zl // 2)
    with scope("greet"):
        pl.semaphore_wait(barrier, len(peers) + N_SEQ - 1)
    pump(0, 0)
    pump(0, 1)
    loads[0].wait()
    loads[1].wait()
    for b in range(2):
        rows = lat[pl.ds(b * 128, 128)].astype(F32)
        xs[me, b] = (layer_norm(rows) * (1.0 + mod[1, b : b + 1]) + mod[0, b : b + 1]).astype(BF16)
        ag_step(0, b)
    pump(1, 0)
    loads[2].wait()
    take_core(zl, 0)
    project(zl, 0)
    pump(1, 1)
    take_core(zl, 1)
    project(zl, 1)
    pump(2, 0)
    pump(2, 1)
    pump(3, 0)
    ag_step(1, 0)
    pump(3, 1)
    take_core(near, 0)
    project(near, 0)
    ag_step(1, 1)
    take_core(near, 1)
    project(near, 1)
    ag_step(2, 0)
    pump(0, 2)
    pump(4, 0)
    take_core(middle, 0)
    project(middle, 0)
    ag_step(2, 1)
    pump(0, 3)
    pump(0, 4)
    take_core(middle, 1)
    project(middle, 1)
    pump(4, 1)
    pump(1, 2)
    ag_step(3, 0)
    take_core(far, 0)
    pump(5, 0)
    project(far, 0)
    attend(0, 0)
    pump(2, 2)
    attend(0, 1)
    ag_step(3, 1)
    pump(3, 2)
    take_core(far, 1)
    pump(5, 1)
    pump(6, 0)
    pump(6, 1)
    project(far, 1)
    attend(1, 0)
    attend(1, 1)
    pump(1, 3)
    pump(1, 4)
    pump(7, 0)
    pump(7, 1)
    with scope("take_heads"):
        for b in range(2):
            bytes_of(heads.at[b, 0:7], h_recv.at[b])
    finish(0)
    finish(1)
    pump(4, 2)
    pump(2, 3)
    pump(2, 4)
    pump(3, 3)
    with scope("take_1"):
        take_rows(nrm, rows_in, x_sem.at[1])
    pump(8, 0)
    pump(8, 1)
    with scope("temporal"):
        temporal()
    send_rows(rows_out, rows_back, x_sem.at[2], x_sem.at[3], -1)
    pump(3, 4)
    pump(4, 3)
    pump(4, 4)
    with scope("take_2"):
        take_rows(rows_out, rows_back, x_sem.at[3])
    with scope("entry"):
        mlp_entry()
        half_copy().start()
    pump(5, 2)
    with scope("mlp"):
        total[c] = mlp_round(0, c)
        half_copy().wait_recv()
        total[1 - c] = mlp_round(0, 1 - c)
    pump(5, 3)
    with scope("mlp"):
        total[c] = mlp_round(1, c)
        total[1 - c] = mlp_round(1, 1 - c)
    pump(5, 4)
    with scope("mlp"):
        part_out[...] = mlp_round(2, 1 - c).astype(BF16)
        part_copy().start()
        total[c] = mlp_round(2, c)
    with scope("last"):
        part_copy().wait_recv()
        for b in range(2):
            rows = pl.ds(b * 128, 128)
            out = (total[c, rows] + part_in[rows].astype(F32)).astype(BF16).astype(F32)
            result[rows] = (mid[rows] + mod[8, b : b + 1] * out).astype(BF16)

    with scope("drain"):
        half_copy().wait_send()
        part_copy().wait_send()
        bytes_of(nrm.at[0:31], x_sem.at[0])
        bytes_of(rows_out.at[0:31], x_sem.at[2])
        ag_drain()
        for b in range(2):
            bytes_of(ot.at[b, 0:7], h_send.at[b])
        for k in range(ROUNDS):
            bytes_of(s1_bytes(k), s1_send.at[k])
            for stage in range(4):
                bytes_of(ring_bytes(stage, k), w_send.at[stage, k])
            if k < ATT:
                for part in range(3):
                    core_copy(k, part).wait_send()


def body(
    latent,
    modulation,
    qkv_spatial,
    gain_spatial,
    out_spatial,
    qkv_temporal,
    gain_temporal,
    out_temporal,
    fc_in,
    fc_out,
):
    vmem = pl.BlockSpec(memory_space=pltpu.VMEM)
    hbm = pl.BlockSpec(memory_space=pl.ANY)
    dma = pltpu.SemaphoreType.DMA
    result = pl.pallas_call(
        block_kernel,
        name="block",
        out_shape=pltpu.VMEM((256, D), BF16),
        in_specs=[hbm] * 2 + [vmem] * 2 + [hbm] * 6,
        out_specs=vmem,
        scratch_shapes=[
            pltpu.VMEM((256, D), BF16),
            pltpu.VMEM((9, 2, D), F32),
            pltpu.VMEM((3, HW, D), BF16),
            dma((3,)),
            pltpu.VMEM((N_TP, 2, 128, D), BF16),
            pltpu.VMEM((2, N_TP, 128, HW), BF16),
            pltpu.VMEM((2, N_TP, HW, 128), BF16),
            pltpu.VMEM((2, HW, 1024), BF16),
            pltpu.VMEM((2, N_TP, HW, 128), BF16),
            pltpu.VMEM((2, N_TP, HW, 128), BF16),
            pltpu.VMEM((4, 2, 4, 4, ATT, 24, D), BF16),
            *[pltpu.VMEM((4, 4, 4, rows, D), BF16) for rows in MLP_ROWS],
            pltpu.VMEM((256, D), F32),
            pltpu.VMEM((N_SEQ, 8, D), BF16),
            pltpu.VMEM((N_SEQ, 8, D), BF16),
            pltpu.VMEM((N_SEQ, 8, D), BF16),
            pltpu.VMEM((N_SEQ, 8, D), BF16),
            pltpu.VMEM((N_TP, HW, 256), BF16),
            pltpu.VMEM((2, 256, D), BF16),
            pltpu.VMEM((2, 256, D), F32),
            pltpu.VMEM((256, D), BF16),
            pltpu.VMEM((256, D), BF16),
            dma((3,)),
            dma((N_TP, 2)),
            dma((ROUNDS,)),
            dma((ROUNDS,)),
            dma((ROUNDS,)),
            dma((4, ROUNDS)),
            dma((4, ROUNDS)),
            dma((ATT, 3)),
            dma((ATT, 3)),
            dma((2,)),
            dma((2,)),
            dma((4,)),
            dma((2,)),
            dma((2,)),
        ],
        compiler_params=pltpu.CompilerParams(
            collective_id=0, has_side_effects=True, vmem_limit_bytes=54 << 20
        ),
    )(
        latent.reshape(256, D),
        modulation.transpose(1, 0, 2),
        gain_spatial,
        gain_temporal,
        qkv_spatial.transpose(0, 2, 1),
        out_spatial.reshape(3, ATT, 24, D),
        qkv_temporal.transpose(0, 2, 1).reshape(9, ATT, 24, D),
        out_temporal.reshape(3, ATT, 24, D),
        fc_in.T.reshape(2, 4, 72, D),
        fc_out.reshape(2, 4, 72, D),
    )
    return result.reshape(latent.shape)


def solution(mesh):
    placed = (
        P(None, "seq", "tp", None),
        P(),
        P(None, None, "tp"),
        P(),
        P("tp", None),
        P(None, None, "tp"),
        P(),
        P("tp", None),
        P(None, "tp"),
        P("tp", None),
    )
    return jax.shard_map(
        body, mesh=mesh, in_specs=placed, out_specs=P(None, "seq", "tp", None), check_vma=False
    )
```

```python
import math

import jax
import jax.numpy as jnp
from jax import lax
from jax.experimental import pallas as pl
from jax.experimental.pallas import tpu as pltpu
from jax.sharding import PartitionSpec as P

D = 1152
H = 16
HD = 72
HW = 144
N_TP = 8
N_SEQ = 32
MESH = pl.DeviceIdType.MESH
EPS = 1e-06
SCALE = 1.0 / math.sqrt(HD)
F32 = jnp.float32
BF16 = jnp.bfloat16

ATT = 2
MLP_ROWS = (32, 24, 16)
ROUNDS = ATT + len(MLP_ROWS)


def layer_norm(values):
    average = jnp.mean(values, axis=-1, keepdims=True)
    centred = values - average
    variance = jnp.mean(centred * centred, axis=-1, keepdims=True)
    return centred * lax.rsqrt(variance + EPS)


def dot(left, right, left_dim=1, right_dim=0):
    return lax.dot_general(
        left, right, (((left_dim,), (right_dim,)), ((), ())), preferred_element_type=F32
    )


def head_norm_rows(values, gain):
    halves = []
    for head in range(2):
        part = values[head * HD : (head + 1) * HD]
        halves.append(part * lax.rsqrt(jnp.mean(part * part, axis=0, keepdims=True) + EPS))
    return jnp.concatenate(halves, axis=0) * gain


def head_norm_lanes(values, gain):
    first = lax.broadcasted_iota(jnp.int32, values.shape, 1) < HD
    square = values * values
    low = jnp.sum(jnp.where(first, square, 0.0), axis=-1, keepdims=True)
    high = jnp.sum(jnp.where(first, 0.0, square), axis=-1, keepdims=True)
    factor = jnp.where(
        first, lax.rsqrt(low * (1.0 / HD) + EPS), lax.rsqrt(high * (1.0 / HD) + EPS)
    )
    return values * factor * gain


def remote(src, dst, send_sem, recv_sem, seq, tp):
    return pltpu.make_async_remote_copy(
        src_ref=src,
        dst_ref=dst,
        send_sem=send_sem,
        recv_sem=recv_sem,
        device_id={"seq": seq, "tp": tp},
        device_id_type=MESH,
    )


def scope(name):
    return jax.named_scope(name)


def block_kernel(
    lat_in,
    mod_in,
    gain_s,
    gain_t,
    wqkv_in,
    src_os,
    src_qkv,
    src_ot,
    src_1,
    src_2,
    result,
    lat,
    mod,
    wqkv,
    in_sem,
    xs,
    ks,
    qs,
    vs,
    ot,
    heads,
    ga,
    gm0,
    gm1,
    gm2,
    mid,
    nrm,
    rows_in,
    rows_out,
    rows_back,
    tt,
    nm,
    total,
    part_out,
    part_in,
    ag_send,
    ag_recv,
    s1_send,
    s1_recv,
    own_sem,
    w_send,
    w_recv,
    d_send,
    d_recv,
    h_send,
    h_recv,
    x_sem,
    m_send,
    m_recv,
):
    seq, me = lax.axis_index("seq"), lax.axis_index("tp")
    x, zh, y = seq // 8, lax.rem(seq // 4, 2), lax.rem(seq, 4)
    zl, c = me // 2, lax.rem(me, 2)
    sib = zl * 2 + (1 - c)
    unit = x * 4 + y

    def xy(dx, dy):
        return (lax.rem(x + dx + 4, 4) * 2 + zh) * 4 + lax.rem(y + dy + 4, 4)

    def zdev(dz):
        z = lax.rem(zh * 4 + zl + dz + 8, 8)
        return (x * 2 + z // 4) * 4 + y, lax.rem(z, 4) * 2 + c

    ring = (xy(1, 0), xy(-1, 0), xy(0, 1), xy(0, -1))
    peers = [(seq, lax.rem(me + i, N_TP)) for i in range(1, N_TP)]
    peers += [zdev(dz) for dz in (1, -1, 2, -2)]
    barrier = pltpu.get_barrier_semaphore()

    def signal(to_seq, to_tp):
        pl.semaphore_signal(
            barrier, inc=1, device_id={"seq": to_seq, "tp": to_tp}, device_id_type=MESH
        )

    for to_seq, to_tp in peers:
        signal(to_seq, to_tp)
    loads = [
        pltpu.make_async_copy(src, dst, in_sem.at[i])
        for i, (src, dst) in enumerate(((lat_in, lat), (mod_in, mod), (wqkv_in, wqkv)))
    ]
    for load in loads:
        load.start()

    def signal_seq(i, _):
        signal(lax.rem(seq + i, N_SEQ), me)
        return 0

    lax.fori_loop(1, N_SEQ, signal_seq, 0)

    def bytes_of(ref, sem):
        pltpu.make_async_copy(ref, ref, sem).wait()

    gm = (gm0, gm1, gm2)

    def spot(k, zs, xi, yi, core=c):
        return ga.at[zs, core, xi, yi, k] if k < ATT else gm[k - ATT].at[zs, xi, yi]

    far_z = (zl // 2) * 4 - 2

    def s1_start(k):
        if k < ATT:
            tables = ((src_os, 0, 3), (src_qkv, 3, 12), (src_ot, 12, 16))
        else:
            tables = ((src_1, 0, 8), (src_2, 8, 16))
        for table, first, last in tables:

            @pl.when((unit >= first) & (unit < last))
            def _():
                if k < ATT:
                    src = table.at[jnp.clip(unit - first, 0, table.shape[0] - 1), k]
                else:
                    rows = pl.ds(sum(MLP_ROWS[: k - ATT]), MLP_ROWS[k - ATT])
                    src = table.at[lax.rem(x, 2), y, rows]
                dst = spot(k, zl, x, y)
                pltpu.make_async_copy(src, dst, own_sem.at[k]).start()
                for dz in (1, -1, far_z):
                    remote(src, dst, s1_send.at[k], s1_recv.at[k], *zdev(dz)).start()

    def s1_bytes(k):
        return spot(k, slice(0, 3), 0, 0, 0)

    def s1_wait(k):
        bytes_of(spot(k, 0, 0, 0, 0), own_sem.at[k])
        bytes_of(s1_bytes(k), s1_recv.at[k])

    x_back, x_next = lax.rem(x + 3, 4), lax.rem(x + 1, 4)
    y_back, y_next = lax.rem(y + 3, 4), lax.rem(y + 1, 4)
    low, high = pl.ds(0, 2), pl.ds(2, 2)
    every = slice(None)

    def ring_copies(stage, k):
        if stage == 0:
            spots = [spot(k, low, x, y)] * 2 + [spot(k, high, x, y)] * 2
        elif stage == 1:
            spots = [
                spot(k, 0, x_back, y),
                spot(k, 1, x_next, y),
                spot(k, 2, x, y_back),
                spot(k, 3, x, y_next),
            ]
        elif stage == 2:
            spots = [spot(k, high, x, every)] * 2 + [spot(k, low, every, y)] * 2
        else:
            spots = [
                spot(k, 2, x_back, every),
                spot(k, 3, x_next, every),
                spot(k, 0, every, y_back),
                spot(k, 1, every, y_next),
            ]
        return [
            remote(there, there, w_send.at[stage, k], w_recv.at[stage, k], ring[i], me)
            for i, there in enumerate(spots)
        ]

    def ring_start(stage, k):
        for copy in ring_copies(stage, k):
            copy.start()

    def ring_wait(stage, k):
        bytes_of(ring_bytes(stage, k), w_recv.at[stage, k])

    def ring_bytes(stage, k):
        pair = slice(0, 2)
        if stage == 0:
            return spot(k, every, 0, pair, 0)
        if stage == 1:
            return spot(k, every, 0, 0, 0)
        return spot(k, every, pair if stage == 2 else 0, every, 0)

    def core_copy(k, part):
        there = (
            ga.at[:, c, 0, 0:3, k],
            ga.at[:, c, 0, 3, k],
            ga.at[:, c, 1:4, :, k],
        )[part]
        return remote(there, there, d_send.at[k, part], d_recv.at[k, part], seq, sib)

    def pump(step, k):
        with scope(f"pump_{step}_{k}"):
            if step == 0:
                s1_start(k)
            elif step == 1:
                s1_wait(k)
                ring_start(0, k)
            elif step <= 4:
                ring_wait(step - 2, k)
                ring_start(step - 1, k)
            elif step == 5:
                ring_wait(3, k)
                if k < ATT:
                    core_copy(k, 0).start()
            elif step == 6:
                core_copy(k, 1).start()
                core_copy(k, 2).start()
            elif step == 7:
                core_copy(k, 0).wait_recv()
            else:
                core_copy(k, 1).wait_recv()
                core_copy(k, 2).wait_recv()

    def ag_copy(slot, b, way):
        to = (jnp.minimum(zl + 1, 3) * 2 + c, jnp.maximum(zl - 1, 0) * 2 + c, sib)[way]
        there = xs.at[slot, b]
        return remote(there, there, ag_send.at[way], ag_recv.at[slot, b], seq, to)

    def ag_step(distance, b):
        with scope(f"ag_{distance}_{b}"):
            ag_now(distance, b)

    def ag_now(distance, b):
        for way in range(2):
            origin = zl - distance if way == 0 else zl + distance
            there = (zl >= distance) if way == 0 else (zl + distance <= 3)
            more = (zl < 3) if way == 0 else (zl > 0)
            slot = origin * 2 + c

            @pl.when(there)
            def _():
                if distance > 0:
                    ag_copy(slot, b, 2).wait_recv()

                @pl.when(more)
                def _():
                    ag_copy(slot, b, way).start()

                if distance > 0 or way == 0:
                    ag_copy(slot, b, 2).start()

    def ag_drain():
        bytes_of(xs.at[0:4], ag_send.at[2])
        for z in range(4):

            @pl.when(zl == z)
            def _():
                if z < 3:
                    bytes_of(xs.at[0 : z + 1], ag_send.at[0])
                if z > 0:
                    bytes_of(xs.at[0 : 4 - z], ag_send.at[1])

    def diagonal(n):
        return lax.broadcasted_iota(jnp.int32, (n, n), 0) == lax.broadcasted_iota(
            jnp.int32, (n, n), 1
        )

    def gain_column(gains, i):
        column = jnp.where(diagonal(HD), gains[i : i + 1], 0.0)
        column = jnp.sum(column, axis=1, keepdims=True)
        return jnp.concatenate([column, column], axis=0)

    def gain_row(gains, i):
        return jnp.sum(
            jnp.where(diagonal(HW), gain_column(gains, i), 0.0), axis=0, keepdims=True
        )

    query_gain, key_gain = gain_column(gain_s, 0), gain_row(gain_s, 1)

    def project(z, b):
        with scope("project"):
            rows = xs[pl.ds(z * 2, 2), b].reshape(256, D)
            queries = head_norm_rows(dot(wqkv[0], rows, 1, 1), query_gain).astype(BF16)
            values = dot(wqkv[2], rows, 1, 1).astype(BF16)
            keys = head_norm_lanes(dot(rows, wqkv[1], 1, 1), key_gain).astype(BF16)
            for core in range(2):
                at = core * 128
                qs[b, z * 2 + core] = queries[:, at : at + 128]
                there = pl.ds(pl.multiple_of((z * 2 + core) * 128, 128), 128)
                vs[b, :, there] = values[:, at : at + 128]
                ks[b, z * 2 + core] = keys[at : at + 128]

    def take_core(z, b):
        ag_copy(z * 2 + (1 - c), b, 2).wait_recv()

    def head_copy(b, to):
        return remote(
            ot.at[b, to], heads.at[b, me], h_send.at[b], h_recv.at[b], seq, to
        )

    def attend(b, half):
        with scope(f"attend_{b}_{half}"):
            attend_now(b, half)

    def attend_now(b, half):
        keys = ks[b].reshape(N_TP * 128, HW)
        values = vs[b]

        def block(i):
            to = lax.rem(me + 1 + i, N_TP)
            query = qs[b, to].astype(F32)
            zero = jnp.zeros((HD, 128), F32)
            pair = jnp.concatenate(
                [
                    jnp.concatenate([query[:HD], zero], axis=0),
                    jnp.concatenate([zero, query[HD:]], axis=0),
                ],
                axis=1,
            ).astype(BF16)
            weights = jnp.exp(dot(keys, pair) * SCALE)
            norm = jnp.sum(weights, axis=0, keepdims=True)
            mixed = dot(values, weights.astype(BF16)) / norm
            out = jnp.concatenate([mixed[:HD, :128], mixed[HD:, 128:]], axis=0).astype(BF16)

            @pl.when(to != me)
            def _():
                ot[b, to] = out
                head_copy(b, to).start()

            @pl.when(to == me)
            def _():
                heads[b, me] = out

        def one_block(i, _):
            block(i)
            return 0

        lax.fori_loop(half * 4, half * 4 + 4, one_block, 0)

    def send_rows(source, target, send, recv, b):
        for other in (1, 0):

            def start(i, _):
                to_x, to_y = lax.rem(x + i // 4, 4), lax.rem(y + i, 4)
                to = (to_x * 2 + lax.rem(zh + other, 2)) * 4 + to_y

                @pl.when((to // 16 == b) | (b < 0))
                def _():
                    remote(source.at[to], target.at[seq], send, recv, to, me).start()

                return 0

            lax.fori_loop(1 - other, 16, start, 0)

    def take_rows(source, target, recv):
        target[seq] = source[seq]
        bytes_of(target.at[0:31], recv)

    def finish(b):
        with scope(f"finish_{b}"):
            mixed = heads[b].reshape(D, 128).T
            out = dot(mixed, ga[:, :, 0, 0:3].reshape(D, D)).astype(BF16).astype(F32)
            rows = pl.ds(b * 128, 128)
            late = lat[rows].astype(F32) + mod[2, b : b + 1] * out
            mid[rows] = late
            normed = layer_norm(late) * (1.0 + mod[4, b : b + 1]) + mod[3, b : b + 1]
            nrm[pl.ds(b * 16, 16)] = normed.reshape(16, 8, D).astype(BF16)
            send_rows(nrm, rows_in, x_sem.at[0], x_sem.at[1], b)

    def att_rows(z, core, first):
        return jnp.concatenate(
            [ga[z, core, u // 4, u % 4].reshape(48, D) for u in range(first, first + 3)], axis=0
        )

    def temporal():
        rows = rows_in[...].astype(F32).reshape(256, D).astype(BF16)
        same = lax.rem(lax.broadcasted_iota(jnp.int32, (256, 256), 0), 8) == lax.rem(
            lax.broadcasted_iota(jnp.int32, (256, 256), 1), 8
        )
        column, row = gain_column(gain_t, 0), gain_row(gain_t, 1)
        zero = jnp.zeros((HD, 256), F32)

        def pair_of_heads(t):
            z, core = t // 2, lax.rem(t, 2)
            table = jnp.concatenate([att_rows(z, core, 3), att_rows(z, core, 9)], axis=0)
            both = dot(table, rows, 1, 1)
            queries = head_norm_rows(both[:HW], column)
            keys = head_norm_lanes(dot(rows, att_rows(z, core, 6), 1, 1), row).astype(BF16)
            values = both[HW:].astype(BF16)
            parts = []
            for head in range(2):
                kept = queries[head * HD : (head + 1) * HD]
                kept = jnp.concatenate([kept, zero] if head == 0 else [zero, kept], axis=0)
                probs = jnp.where(same, jnp.exp(dot(keys, kept.astype(BF16)) * SCALE), 0.0)
                norm = jnp.sum(probs, axis=0, keepdims=True)
                mixed = dot(values, probs.astype(BF16)) / norm
                parts.append(mixed[head * HD : (head + 1) * HD])
            return jnp.concatenate(parts, axis=0).astype(BF16)

        def four_pairs(i, _):
            done = [pair_of_heads(4 * i + j) for j in range(4)]
            for j in range(4):
                tt[4 * i + j] = done[j]
            return 0

        lax.fori_loop(0, 2, four_pairs, 0)
        out = dot(tt[...].reshape(D, 256).T, ga[:, :, 3, 0:3].reshape(D, D))
        rows_out[...] = out.reshape(N_SEQ, 8, D).astype(BF16)

    def half_copy():
        return remote(nm.at[c], nm.at[c], m_send.at[0], m_recv.at[0], seq, sib)

    def part_copy():
        return remote(part_out, part_in, m_send.at[1], m_recv.at[1], seq, sib)

    def mlp_entry():
        back = rows_back[...].astype(F32).reshape(256, D)
        for b in range(2):
            rows = pl.ds(b * 128, 128)
            late = mid[rows] + mod[5, b : b + 1] * back[b * 128 : (b + 1) * 128]
            mid[rows] = late
            normed = layer_norm(late) * (1.0 + mod[7, b : b + 1]) + mod[6, b : b + 1]
            nm[c, rows] = normed.astype(BF16)

    def mlp_round(k, which):
        u = dot(nm[which], gm[k][:, 0:2].reshape(32 * MLP_ROWS[k], D), 1, 1)
        h = 0.5 * u * (1.0 + jnp.tanh(math.sqrt(2.0 / math.pi) * (u + 0.044715 * (u * u * u))))
        product = dot(h.astype(BF16), gm[k][:, 2:4].reshape(32 * MLP_ROWS[k], D))
        return product if k == 0 else total[which] + product

    near = zl + 1 - 2 * lax.rem(zl, 2)
    middle = 2 - zl // 2
    far = 3 - 3 * (zl // 2)
    with scope("greet"):
        pl.semaphore_wait(barrier, len(peers) + N_SEQ - 1)
    pump(0, 0)
    pump(0, 1)
    loads[0].wait()
    loads[1].wait()
    for b in range(2):
        rows = lat[pl.ds(b * 128, 128)].astype(F32)
        xs[me, b] = (layer_norm(rows) * (1.0 + mod[1, b : b + 1]) + mod[0, b : b + 1]).astype(BF16)
        ag_step(0, b)
    pump(1, 0)
    loads[2].wait()
    take_core(zl, 0)
    project(zl, 0)
    pump(1, 1)
    take_core(zl, 1)
    project(zl, 1)
    pump(2, 0)
    pump(2, 1)
    pump(3, 0)
    ag_step(1, 0)
    pump(3, 1)
    take_core(near, 0)
    project(near, 0)
    ag_step(1, 1)
    take_core(near, 1)
    project(near, 1)
    ag_step(2, 0)
    pump(0, 2)
    pump(4, 0)
    take_core(middle, 0)
    project(middle, 0)
    ag_step(2, 1)
    pump(0, 3)
    pump(0, 4)
    take_core(middle, 1)
    project(middle, 1)
    pump(4, 1)
    pump(1, 2)
    ag_step(3, 0)
    take_core(far, 0)
    pump(5, 0)
    project(far, 0)
    attend(0, 0)
    pump(2, 2)
    attend(0, 1)
    ag_step(3, 1)
    pump(3, 2)
    take_core(far, 1)
    pump(5, 1)
    pump(6, 0)
    pump(6, 1)
    project(far, 1)
    attend(1, 0)
    attend(1, 1)
    pump(1, 3)
    pump(1, 4)
    pump(7, 0)
    pump(7, 1)
    with scope("take_heads"):
        for b in range(2):
            bytes_of(heads.at[b, 0:7], h_recv.at[b])
    finish(0)
    finish(1)
    pump(4, 2)
    pump(2, 3)
    pump(2, 4)
    pump(3, 3)
    with scope("take_1"):
        take_rows(nrm, rows_in, x_sem.at[1])
    pump(8, 0)
    pump(8, 1)
    with scope("temporal"):
        temporal()
    send_rows(rows_out, rows_back, x_sem.at[2], x_sem.at[3], -1)
    pump(3, 4)
    pump(4, 3)
    pump(4, 4)
    with scope("take_2"):
        take_rows(rows_out, rows_back, x_sem.at[3])
    with scope("entry"):
        mlp_entry()
        half_copy().start()
    pump(5, 2)
    with scope("mlp"):
        total[c] = mlp_round(0, c)
        half_copy().wait_recv()
        total[1 - c] = mlp_round(0, 1 - c)
    pump(5, 3)
    with scope("mlp"):
        total[c] = mlp_round(1, c)
        total[1 - c] = mlp_round(1, 1 - c)
    pump(5, 4)
    with scope("mlp"):
        part_out[...] = mlp_round(2, 1 - c).astype(BF16)
        part_copy().start()
        total[c] = mlp_round(2, c)
    with scope("last"):
        part_copy().wait_recv()
        for b in range(2):
            rows = pl.ds(b * 128, 128)
            out = (total[c, rows] + part_in[rows].astype(F32)).astype(BF16).astype(F32)
            result[rows] = (mid[rows] + mod[8, b : b + 1] * out).astype(BF16)

    with scope("drain"):
        half_copy().wait_send()
        part_copy().wait_send()
        bytes_of(nrm.at[0:31], x_sem.at[0])
        bytes_of(rows_out.at[0:31], x_sem.at[2])
        ag_drain()
        for b in range(2):
            bytes_of(ot.at[b, 0:7], h_send.at[b])
        for k in range(ROUNDS):
            bytes_of(s1_bytes(k), s1_send.at[k])
            for stage in range(4):
                bytes_of(ring_bytes(stage, k), w_send.at[stage, k])
            if k < ATT:
                for part in range(3):
                    core_copy(k, part).wait_send()


def body(
    latent,
    modulation,
    qkv_spatial,
    gain_spatial,
    out_spatial,
    qkv_temporal,
    gain_temporal,
    out_temporal,
    fc_in,
    fc_out,
):
    vmem = pl.BlockSpec(memory_space=pltpu.VMEM)
    hbm = pl.BlockSpec(memory_space=pl.ANY)
    dma = pltpu.SemaphoreType.DMA
    result = pl.pallas_call(
        block_kernel,
        name="block",
        out_shape=pltpu.VMEM((256, D), BF16),
        in_specs=[hbm] * 2 + [vmem] * 2 + [hbm] * 6,
        out_specs=vmem,
        scratch_shapes=[
            pltpu.VMEM((256, D), BF16),
            pltpu.VMEM((9, 2, D), F32),
            pltpu.VMEM((3, HW, D), BF16),
            dma((3,)),
            pltpu.VMEM((N_TP, 2, 128, D), BF16),
            pltpu.VMEM((2, N_TP, 128, HW), BF16),
            pltpu.VMEM((2, N_TP, HW, 128), BF16),
            pltpu.VMEM((2, HW, 1024), BF16),
            pltpu.VMEM((2, N_TP, HW, 128), BF16),
            pltpu.VMEM((2, N_TP, HW, 128), BF16),
            pltpu.VMEM((4, 2, 4, 4, ATT, 24, D), BF16),
            *[pltpu.VMEM((4, 4, 4, rows, D), BF16) for rows in MLP_ROWS],
            pltpu.VMEM((256, D), F32),
            pltpu.VMEM((N_SEQ, 8, D), BF16),
            pltpu.VMEM((N_SEQ, 8, D), BF16),
            pltpu.VMEM((N_SEQ, 8, D), BF16),
            pltpu.VMEM((N_SEQ, 8, D), BF16),
            pltpu.VMEM((N_TP, HW, 256), BF16),
            pltpu.VMEM((2, 256, D), BF16),
            pltpu.VMEM((2, 256, D), F32),
            pltpu.VMEM((256, D), BF16),
            pltpu.VMEM((256, D), BF16),
            dma((3,)),
            dma((N_TP, 2)),
            dma((ROUNDS,)),
            dma((ROUNDS,)),
            dma((ROUNDS,)),
            dma((4, ROUNDS)),
            dma((4, ROUNDS)),
            dma((ATT, 3)),
            dma((ATT, 3)),
            dma((2,)),
            dma((2,)),
            dma((4,)),
            dma((2,)),
            dma((2,)),
        ],
        compiler_params=pltpu.CompilerParams(
            collective_id=0, has_side_effects=True, vmem_limit_bytes=54 << 20
        ),
    )(
        latent.reshape(256, D),
        modulation.transpose(1, 0, 2),
        gain_spatial,
        gain_temporal,
        qkv_spatial.transpose(0, 2, 1),
        out_spatial.reshape(3, ATT, 24, D),
        qkv_temporal.transpose(0, 2, 1).reshape(9, ATT, 24, D),
        out_temporal.reshape(3, ATT, 24, D),
        fc_in.T.reshape(2, 4, 72, D),
        fc_out.reshape(2, 4, 72, D),
    )
    return result.reshape(latent.shape)


def solution(mesh):
    placed = (
        P(None, "seq", "tp", None),
        P(),
        P(None, None, "tp"),
        P(),
        P("tp", None),
        P(None, None, "tp"),
        P(),
        P("tp", None),
        P(None, "tp"),
        P("tp", None),
    )
    return jax.shard_map(
        body, mesh=mesh, in_specs=placed, out_specs=P(None, "seq", "tp", None), check_vma=False
    )
```
